32 devices in a mesh: gz: 2 (over core), dp: 16 (over z, y, x).
Axes of the slice: x: 2, y: 2, z: 4, core: 2. Of those that a mesh axis runs over, the one named last changes fastest.
Arguments:
- inputs: bfloat16 [16, 32, 16, 8, 128], P('dp', None, 'gz'), may hold values from -6 to 6
- kernel_one: bfloat16 [32, 32, 3, 3, 3], replicated, may hold values from -0.21875 to 0.21875
- kernel_two: bfloat16 [32, 32, 3, 3, 3], replicated, may hold values from -0.21875 to 0.21875
- cotangent: bfloat16 [16, 32, 16, 8, 128], P('dp', None, 'gz'), may hold values from -12 to 12
Outputs:
- input_grad: bfloat16 [16, 32, 16, 8, 128], P('dp', None, 'gz')
- kernel_one_grad: float32 [32, 32, 3, 3, 3], replicated
- kernel_two_grad: float32 [32, 32, 3, 3, 3], replicated
The draws below stay inside these ranges and needn't reach their ends.
All inputs are finite; a program needn't handle non-finite values.
Results may differ from the reference program's by a relative error of at most 0.006.
Values may be sent and summed in bfloat16 or wider, within the bound.
No kernel may reach another device: no remote copies, remote signals or barrier semaphores. Data moves between devices by JAX's collectives and lax.ppermute only.
A program may use at most 64 MiB of HBM per device.

```python
import math
import jax
import jax.numpy as jnp
from jax import lax

C = 32
NY = 8
NX = 128
NZ = 16
BATCH = 16


def draw_cotangent(key, part):
    sample_pos = jnp.arange(BATCH, dtype=jnp.float32) / max(BATCH - 1, 1)
    plane_pos = jnp.arange(NZ, dtype=jnp.float32) / max(NZ - 1, 1)
    scale = 1.0 + sample_pos[:, None, None, None, None] + plane_pos[None, None, :, None, None]
    base = jnp.clip(jax.random.normal(key, (BATCH, C, NZ, NY, NX), jnp.float32), -4.0, 4.0)
    return (base * scale).astype(jnp.bfloat16)


def steps_of(stream_key, extent, split, low, high):
    def one(position, parts):
        draws = jax.random.uniform(jax.random.fold_in(jax.random.fold_in(stream_key, 6), position), (parts,), jnp.float32, low / len(split), high / len(split))
        return jnp.repeat(jnp.exp(draws), extent[position] // parts).reshape((-1,) + (1,) * (len(extent) - position - 1))

    gain = one(*split[0])
    for cut in split[1:]:
        gain = gain * one(*cut)
    return gain


def normal_values(rng, extent, spread, most, pieces=(), held_as=jnp.bfloat16):
    entries = spread * jax.random.normal(rng, extent, jnp.float32)
    if pieces:
        entries = entries * steps_of(rng, extent, pieces, -0.22, 0.18)
    return jnp.clip(entries, -most, most).astype(held_as)


def setup_inputs(seed: int = 0) -> dict:
    streams_of = jax.random.split(jax.random.key(seed), 5)
    return {
        "inputs": normal_values(streams_of[0], (BATCH, C, NZ, NY, NX), 1.0, 6.0, ((0, 16), (2, 2))),
        "kernel_one": normal_values(streams_of[1], (C, C, 3, 3, 3), (27 * C) ** -0.5, 0.21875),
        "kernel_two": normal_values(streams_of[2], (C, C, 3, 3, 3), (27 * C) ** -0.5, 0.21875),
        "cotangent": draw_cotangent(jax.random.fold_in(streams_of[4], 71), 0),
    }


def convolve(field, kernel):
    out = lax.conv_general_dilated(field[None], kernel, (1, 1, 1), ((1, 1), (1, 1), (1, 1)), dimension_numbers=('NCDHW', 'OIDHW', 'NCDHW'), preferred_element_type=jnp.float32)
    return out[0]

def flipped(kernel):
    return jnp.swapaxes(jnp.flip(kernel, (2, 3, 4)), 0, 1)

def kernel_terms(padded, grad):
    out = lax.conv_general_dilated(padded[None], grad[None], (1, 1, 1), 'VALID', dimension_numbers=('CNDHW', 'IODHW', 'NCDHW'), preferred_element_type=jnp.float32)
    return jnp.transpose(out, (1, 0, 2, 3, 4))

def dsilu(value):
    sig = jax.nn.sigmoid(value)
    return sig * (1.0 + value * (1.0 - sig))

def one_sample(pair, kernel_one, kernel_two):
    source, upstream = pair
    pre_one = convolve(source, kernel_one)
    hidden = jax.nn.silu(pre_one).astype(jnp.bfloat16)
    pre_two = convolve(hidden, kernel_two)
    grad_two = (upstream.astype(jnp.float32) * dsilu(pre_two)).astype(jnp.bfloat16)
    hidden_grad = convolve(grad_two, flipped(kernel_two))
    grad_one = (hidden_grad * dsilu(pre_one)).astype(jnp.bfloat16)
    input_grad = convolve(grad_one, flipped(kernel_one)).astype(jnp.bfloat16)
    widths = ((0, 0), (1, 1), (1, 1), (1, 1))
    term_two = kernel_terms(jnp.pad(hidden, widths), grad_two)
    term_one = kernel_terms(jnp.pad(source, widths), grad_one)
    return (input_grad, term_one, term_two)

def reference(inputs, kernel_one, kernel_two, cotangent):
    input_grad, terms_one, terms_two = lax.map(lambda pair: one_sample(pair, kernel_one, kernel_two), (inputs, cotangent))
    factor = 1.0 / math.sqrt(BATCH * NZ * NY * NX)
    return (input_grad, lax.optimization_barrier(jnp.sum(terms_one, axis=0)) * factor, lax.optimization_barrier(jnp.sum(terms_two, axis=0)) * factor)
```

```python
import functools
import math

import jax
import jax.numpy as jnp
from jax import lax
from jax.experimental import pallas as pl
from jax.experimental.pallas import tpu as pltpu
from jax.sharding import PartitionSpec as P

F32, BF16 = jnp.float32, jnp.bfloat16
NT = (((1,), (1,)), ((), ()))
REACH = 4


def params(mib):
    return pltpu.CompilerParams(vmem_limit_bytes=mib * 2**20)


def cost(flops, size):
    return pl.CostEstimate(flops=int(flops), bytes_accessed=int(size), transcendentals=0)


def prep_kernel(mirrored, one_ref, two_ref, *refs):
    flip = lax.axis_index("gz") == 1 if mirrored else False
    outs, wide = refs[:4], refs[4]
    chan = one_ref.shape[-1]
    full = outs[0].shape[1]
    height = full // chan
    lane = lax.broadcasted_iota(jnp.int32, (chan, full), 1)
    row = lax.broadcasted_iota(jnp.int32, (chan, full), 0)
    repeat = jnp.where(lax.rem(lane, chan) == row, 1.0, 0.0).astype(BF16)
    block = lane // chan
    for index, ref in enumerate((one_ref, two_ref)):
        forward, backward = outs[2 * index], outs[2 * index + 1]
        flat = ref[...].reshape(27 * chan, chan)
        spread = jnp.dot(flat, repeat, preferred_element_type=F32)
        wide[...] = spread.reshape(3, 9 * chan, full)
        for dz in range(3):
            source = jnp.where(flip, 2 - dz, dz) if mirrored else dz
            for dx in range(3):
                taps = [
                    wide[source, (dy * 3 + dx) * chan : (dy * 3 + dx + 1) * chan, :]
                    for dy in range(3)
                ]
                strips = []
                for y in range(height):
                    strip = jnp.zeros((chan, full), F32)
                    for dy in range(3):
                        strip = jnp.where(block == y + dy - 1, taps[dy], strip)
                    strips.append(strip.astype(BF16))
                tile = jnp.concatenate(strips, axis=0)
                forward[dz, :, dx * full : (dx + 1) * full] = tile
                backward[2 - dz, :, (2 - dx) * full : (3 - dx) * full] = tile.T


class Field:
    def __init__(self, ref, base, full, width):
        self.ref, self.base, self.full, self.width = ref, base, full, width

    def lanes(self, first, count):
        start = (first + self.base) * self.width
        return slice(start, start + count * self.width)

    def put(self, plane, value):
        full, width = self.full, self.width
        lane = lax.broadcasted_iota(jnp.int32, (full, width), 1)
        before = jnp.where(lane == 0, 0.0, pltpu.roll(value, 1, 1))
        after = jnp.where(lane == width - 1, 0.0, pltpu.roll(value, width - 1, 1))
        for dx, item in enumerate((before, value, after)):
            self.ref[dx * full : (dx + 1) * full, self.lanes(plane, 1)] = item.astype(BF16)

    def blank(self, plane):
        self.ref[:, self.lanes(plane, 1)] = jnp.zeros((3 * self.full, self.width), BF16)

    def convolve(self, band, first, count):
        total = None
        for dz in range(3):
            piece = jnp.dot(
                band[dz], self.ref[:, self.lanes(first + dz - 1, count)], preferred_element_type=F32
            )
            total = piece if total is None else total + piece
        return total


def spans(low, high):
    return [(at, min(2, high - at)) for at in range(low, high, 2)]


def sigmoid(value):
    return 0.5 * jnp.tanh(0.5 * value) + 0.5


def gradient(field, own, grad_ref, out_ref, planes, chan, flip):
    full, width = field.full, field.width
    height = full // chan
    whole = own + 2
    total = jnp.zeros(out_ref.shape, F32)
    lanes = field.lanes(-1, whole)
    for y in range(height):
        parts = []
        for dz in range(3):
            if flip is None:
                start = (2 - dz) * width
            else:
                start = pl.multiple_of(jnp.where(flip, dz, 2 - dz) * width, width)
            parts.append(grad_ref[y * chan : (y + 1) * chan, pl.ds(start, whole * width)])
        right = jnp.concatenate(parts, axis=0)
        low, high = max(y - 1, 0), min(y + 2, height)
        left = jnp.concatenate(
            [
                field.ref[dx * full + low * chan : dx * full + high * chan, lanes]
                for dx in range(3)
            ],
            axis=0,
        )
        piece = lax.dot_general(left, right, NT, preferred_element_type=F32)
        rows = (high - low) * chan
        if high - low < 3:
            blank = jnp.zeros(((3 - high + low) * chan, piece.shape[1]), F32)
            cut = [piece[dx * rows : (dx + 1) * rows] for dx in range(3)]
            order = [[blank, c] if y == 0 else [c, blank] for c in cut]
            piece = jnp.concatenate([p for pair in order for p in pair], axis=0)
        total = total + piece
    out_ref[...] = total


def main_kernel(count, sizes, *refs):
    chan, own, height, width, low_side, high_side = sizes
    full = chan * height
    mirrored = count == 2
    halos = low_side + high_side
    data_ref, cot_ref = refs[:2]
    halo_refs = refs[2 : 2 + halos]
    band_one, band_two, back_two = refs[2 + halos : 5 + halos]
    grad_field_ref, term_one, term_two = refs[5 + halos : 8 + halos]
    x_ref, h_ref, g_ref, own_ref, slope_ref, turn_ref = refs[8 + halos :]
    position = lax.axis_index("gz")
    flip = position == 1 if mirrored else None

    def reach(depth):
        return (-depth * low_side, own + depth * high_side)

    def field(ref, depth):
        item = Field(ref, depth if low_side else 1, full, width)
        if not low_side:
            item.blank(-1)
        if not high_side:
            item.blank(own)
        return item

    def turned(slot, value):
        turn_ref[slot] = value.astype(F32).reshape(full, width)
        return jnp.concatenate(
            [turn_ref[slot, pl.ds(y, chan, stride=height), :] for y in range(height)], axis=0
        )

    def plane_of(ref, plane, skip, depth):
        if 0 <= plane < own:
            at = jnp.where(flip, own - 1 - plane, plane) if mirrored else plane
            return ref[:, at]
        if plane < 0:
            return halo_refs[0][:, skip + depth + plane]
        at = plane - own
        if mirrored:
            at = jnp.where(flip, depth - 1 - at, at)
        return halo_refs[-1][:, skip + at]

    def kept(plane, value):
        if count == 2:
            return value
        if plane < 0:
            return jnp.where(position > 0, value, 0.0)
        if plane >= own:
            return jnp.where(position < count - 1, value, 0.0)
        return value

    data = field(x_ref, REACH)
    for plane in range(*reach(REACH)):
        data.put(plane, turned(plane % 2, plane_of(data_ref, plane, 0, REACH)))

    hidden = field(h_ref, REACH - 1)
    slope_low, slope_high = reach(1)
    for first, number in spans(*reach(REACH - 1)):
        pre = data.convolve(band_one, first, number)
        for step in range(number):
            plane = first + step
            value = pre[:, step * width : (step + 1) * width]
            gate = sigmoid(value)
            hidden.put(plane, kept(plane, value * gate))
            if slope_low <= plane < slope_high:
                at = (plane - slope_low) * width
                slope_ref[:, at : at + width] = gate * (1.0 + value * (1.0 - gate))

    own_ref[:, : 2 * width] = jnp.zeros((full, 2 * width), BF16)
    own_ref[:, (own + 2) * width :] = jnp.zeros((full, 2 * width), BF16)

    upper = field(g_ref, REACH - 2)
    for first, number in spans(*reach(REACH - 2)):
        pre = hidden.convolve(band_two, first, number)
        for step in range(number):
            plane = first + step
            value = pre[:, step * width : (step + 1) * width]
            gate = sigmoid(value)
            seed = turned(plane % 2, plane_of(cot_ref, plane, REACH, REACH - 2))
            grad = seed * (gate * (1.0 + value * (1.0 - gate)))
            upper.put(plane, grad)
            if 0 <= plane < own:
                own_ref[:, (plane + 2) * width : (plane + 3) * width] = grad.astype(BF16)
    gradient(hidden, own, own_ref, term_two, None, chan, flip)

    lower = field(grad_field_ref, REACH - 3)
    for first, number in spans(*reach(REACH - 3)):
        back = upper.convolve(back_two, first, number)
        for step in range(number):
            plane = first + step
            at = (plane - slope_low) * width
            grad = back[:, step * width : (step + 1) * width] * slope_ref[:, at : at + width]
            grad = kept(plane, grad)
            lower.put(plane, grad)
            if 0 <= plane < own:
                own_ref[:, (plane + 2) * width : (plane + 3) * width] = grad.astype(BF16)
    gradient(data, own, own_ref, term_one, None, chan, flip)


def last_kernel(count, sizes, grad_field_ref, back_one, out_ref, turn_ref):
    chan, own, height, width, _, _ = sizes
    full = chan * height
    mirrored = count == 2
    flip = lax.axis_index("gz") == 1 if mirrored else None
    lower = Field(grad_field_ref, 1, full, width)
    for first, number in spans(0, own):
        out = lower.convolve(back_one, first, number)
        for step in range(number):
            plane = first + step
            value = out[:, step * width : (step + 1) * width]
            slot = plane % 2
            for y in range(height):
                turn_ref[slot, pl.ds(y, chan, stride=height), :] = value[y * chan : (y + 1) * chan]
            at = jnp.where(flip, own - 1 - plane, plane) if mirrored else plane
            out_ref[:, at] = turn_ref[slot].reshape(chan, height, width).astype(BF16)


def unpack_kernel(factor, one_ref, two_ref, out_one, out_two):
    chan = out_one.shape[-1]
    for ref, out in ((one_ref, out_one), (two_ref, out_two)):
        value = ref[...].T * factor
        for dz in range(3):
            for dy in range(3):
                for dx in range(3):
                    at = (dx * 3 + dy) * chan
                    out[dz, dy, dx] = value[dz * chan : (dz + 1) * chan, at : at + chan]


def doubled(value, axis):
    count = lax.axis_size(axis)
    if count & (count - 1):
        return lax.psum(value, axis)
    step = 1
    while step < count:
        value = value + lax.ppermute(value, axis, [(i, i ^ step) for i in range(count)])
        step *= 2
    return value


def reduced(one, two):
    if lax.axis_size("gz") == 2:
        swap = [(0, 1), (1, 0)]
        first = lax.axis_index("gz") == 0
        mine = jnp.where(first, two, one)
        mine = mine + lax.ppermute(jnp.where(first, one, two), "gz", swap)
        mine = doubled(mine, "dp")
        other = lax.ppermute(mine, "gz", swap)
        return jnp.where(first, other, mine), jnp.where(first, mine, other)
    both = doubled(doubled(jnp.stack([one, two]), "gz"), "dp")
    return both[0], both[1]


def halo_of(data, cot, count):
    own = data.shape[1]

    def ends(low):
        parts = []
        for value, depth in ((data, REACH), (cot, REACH - 2)):
            start = jnp.where(low, 0, own - depth) if count == 2 else (0 if low else own - depth)
            parts.append(lax.dynamic_slice_in_dim(value, start, depth, axis=1))
        return jnp.concatenate(parts, axis=1)

    if count == 1:
        return []
    if count == 2:
        return [lax.ppermute(ends(lax.axis_index("gz") == 1), "gz", [(0, 1), (1, 0)])]
    up = [(i, i + 1) for i in range(count - 1)]
    down = [(j, i) for i, j in up]
    return [lax.ppermute(ends(False), "gz", up), lax.ppermute(ends(True), "gz", down)]


def local(inputs, kernel_one, kernel_two, cotangent):
    count = lax.axis_size("gz")
    batch, chan, own, height, width = inputs.shape
    full = chan * height
    low_side, high_side = (1, 1) if count > 2 else (0, 1 if count == 2 else 0)
    sizes = (chan, own, height, width, low_side, high_side)
    sides = low_side + high_side
    taps = [jnp.transpose(k, (2, 3, 4, 0, 1)) for k in (kernel_one, kernel_two)]
    bands = pl.pallas_call(
        functools.partial(prep_kernel, count == 2),
        out_shape=[jax.ShapeDtypeStruct((3, full, 3 * full), BF16)] * 4,
        scratch_shapes=[pltpu.VMEM((3, 9 * chan, full), F32)],
        compiler_params=params(16),
        cost_estimate=cost(2e9, 5e6),
        name="prep",
    )(*taps)

    def slots(depth):
        return own + sum(depth if side else 1 for side in (low_side, high_side))

    def stack(depth):
        return (3 * full, slots(depth) * width)

    outs, ones, twos = [], [], []
    for sample in range(batch):
        data, cot = inputs[sample], cotangent[sample]
        halos = halo_of(data, cot, count)
        term = jax.ShapeDtypeStruct((9 * chan, 3 * chan), F32)
        grad_field, term_one, term_two = pl.pallas_call(
            functools.partial(main_kernel, count, sizes),
            out_shape=[jax.ShapeDtypeStruct(stack(REACH - 3), BF16), term, term],
            scratch_shapes=[
                pltpu.VMEM(stack(REACH), BF16),
                pltpu.VMEM(stack(REACH - 1), BF16),
                pltpu.VMEM(stack(REACH - 2), BF16),
                pltpu.VMEM((full, (own + 4) * width), BF16),
                pltpu.VMEM((full, (own + sides) * width), F32),
                pltpu.VMEM((2, full, width), F32),
            ],
            compiler_params=params(32),
            cost_estimate=cost(8e9, 8e6),
            name="main",
        )(data, cot, *halos, bands[0], bands[2], bands[3])
        out = pl.pallas_call(
            functools.partial(last_kernel, count, sizes),
            out_shape=jax.ShapeDtypeStruct((chan, own, height, width), BF16),
            scratch_shapes=[pltpu.VMEM((2, full, width), F32)],
            compiler_params=params(16),
            cost_estimate=cost(2e9, 3e6),
            name="last",
        )(grad_field, bands[1])
        outs.append(out)
        ones.append(term_one)
        twos.append(term_two)
    one, two = reduced(sum(ones[1:], ones[0]), sum(twos[1:], twos[0]))
    cells = lax.axis_size("dp") * batch * count * own * height * width
    grads = pl.pallas_call(
        functools.partial(unpack_kernel, 1.0 / math.sqrt(cells)),
        out_shape=[jax.ShapeDtypeStruct((3, 3, 3, chan, chan), F32)] * 2,
        compiler_params=params(8),
        name="unpack",
    )(one, two)
    one, two = [jnp.transpose(g, (3, 4, 0, 1, 2)) for g in grads]
    return jnp.stack(outs), one, two


def solution(mesh):
    return jax.shard_map(
        local,
        mesh=mesh,
        in_specs=(P("dp", None, "gz", None, None), P(), P(), P("dp", None, "gz", None, None)),
        out_specs=(P("dp", None, "gz", None, None), P(), P()),
        check_vma=False,
    )
```

```python
import functools
import math

import jax
import jax.numpy as jnp
from jax import lax
from jax.experimental import pallas as pl
from jax.experimental.pallas import tpu as pltpu
from jax.sharding import PartitionSpec as P

F32, BF16 = jnp.float32, jnp.bfloat16
NT = (((1,), (1,)), ((), ()))
REACH = 4


def params(mib):
    return pltpu.CompilerParams(vmem_limit_bytes=mib * 2**20)


def cost(flops, size):
    return pl.CostEstimate(flops=int(flops), bytes_accessed=int(size), transcendentals=0)


def pack_kernel(count, own, data_ref, cot_ref, *refs):
    outs, sems = refs[:-1], refs[-1]
    copies = []
    for side, out in enumerate(outs):
        for which, (ref, depth, at) in enumerate(
            ((data_ref, REACH, 0), (cot_ref, REACH - 2, REACH))
        ):
            start = own - depth if side == 0 else 0
            if count == 2:
                start = jnp.where(lax.axis_index("gz") == 1, 0, own - depth)
            copies.append(
                pltpu.make_async_copy(
                    ref.at[:, pl.ds(start, depth)],
                    out.at[:, pl.ds(at, depth)],
                    sems.at[side, which],
                )
            )
    for copy in copies:
        copy.start()
    for copy in copies:
        copy.wait()


def turned(turn_ref, slot, value):
    chan, height, width = value.shape
    turn_ref[slot] = value.astype(F32).reshape(chan * height, width)
    return jnp.concatenate(
        [turn_ref[slot, pl.ds(y, chan, stride=height), :] for y in range(height)], axis=0
    )


def prep_kernel(mirrored, data_ref, one_ref, two_ref, *refs):
    flip = lax.axis_index("gz") == 1 if mirrored else False
    outs, field_ref, wide, turn_ref = refs[:4], refs[4], refs[5], refs[6]
    chan = one_ref.shape[-1]
    full = outs[0].shape[1]
    height = full // chan
    own, width = data_ref.shape[1], data_ref.shape[-1]
    field = Field([(field_ref, 0, own, 0)], full, width)
    for plane in range(own):
        at = jnp.where(flip, own - 1 - plane, plane) if mirrored else plane
        field.put(plane, turned(turn_ref, plane % 2, data_ref[:, at]))
    lane = lax.broadcasted_iota(jnp.int32, (chan, full), 1)
    row = lax.broadcasted_iota(jnp.int32, (chan, full), 0)
    repeat = jnp.where(lax.rem(lane, chan) == row, 1.0, 0.0).astype(BF16)
    block = lane // chan
    for index, ref in enumerate((one_ref, two_ref)):
        forward, backward = outs[2 * index], outs[2 * index + 1]
        flat = ref[...].reshape(27 * chan, chan)
        spread = jnp.dot(flat, repeat, preferred_element_type=F32)
        wide[...] = spread.reshape(3, 9 * chan, full)
        for dz in range(3):
            source = jnp.where(flip, 2 - dz, dz) if mirrored else dz
            for dx in range(3):
                taps = [
                    wide[source, (dy * 3 + dx) * chan : (dy * 3 + dx + 1) * chan, :]
                    for dy in range(3)
                ]
                strips = []
                for y in range(height):
                    strip = jnp.zeros((chan, full), F32)
                    for dy in range(3):
                        strip = jnp.where(block == y + dy - 1, taps[dy], strip)
                    strips.append(strip.astype(BF16))
                tile = jnp.concatenate(strips, axis=0)
                forward[dz, :, dx * full : (dx + 1) * full] = tile
                backward[2 - dz, :, (2 - dx) * full : (3 - dx) * full] = tile.T


class Field:
    def __init__(self, pieces, full, width):
        self.pieces, self.full, self.width = pieces, full, width

    def run(self, plane, count):
        for ref, first, number, base in self.pieces:
            if first <= plane < first + number:
                at = plane - first
                size = min(count, number - at)
                return ref, slice((base + at) * self.width, (base + at + size) * self.width), size
        raise IndexError(plane)

    def take(self, rows, first, count):
        parts = []
        while count:
            ref, lanes, size = self.run(first, count)
            parts.append(ref[rows, lanes])
            first, count = first + size, count - size
        return parts[0] if len(parts) == 1 else jnp.concatenate(parts, axis=1)

    def put(self, plane, value):
        full, width = self.full, self.width
        ref, lanes, _ = self.run(plane, 1)
        lane = lax.broadcasted_iota(jnp.int32, (full, width), 1)
        before = jnp.where(lane == 0, 0.0, pltpu.roll(value, 1, 1))
        after = jnp.where(lane == width - 1, 0.0, pltpu.roll(value, width - 1, 1))
        for dx, item in enumerate((before, value, after)):
            ref[dx * full : (dx + 1) * full, lanes] = item.astype(BF16)

    def blank(self, plane):
        ref, lanes, _ = self.run(plane, 1)
        ref[:, lanes] = jnp.zeros((3 * self.full, self.width), BF16)

    def convolve(self, band, first, count):
        total = None
        for dz in range(3):
            window = self.take(slice(None), first + dz - 1, count)
            piece = jnp.dot(band[dz], window, preferred_element_type=F32)
            total = piece if total is None else total + piece
        return total


def spans(low, high):
    return [(at, min(2, high - at)) for at in range(low, high, 2)]


def sigmoid(value):
    return 0.5 * jnp.tanh(0.5 * value) + 0.5


def gradient(field, grads, own, chan, flip, out_ref):
    full = field.full
    height = full // chan
    sums = [[None] * 3 for _ in range(3)]
    for base in range(0, height, 2):
        right = jnp.concatenate(
            [
                grads.take(slice((2 - dx) * full + y * chan, (2 - dx) * full + (y + 1) * chan), 0, own)
                for y in (base, base + 1)
                for dx in (0, 1, 2, 2)
            ],
            axis=0,
        )
        low, high = max(base - 1, 0), min(base + 3, height)
        left = jnp.concatenate(
            [
                field.take(slice(full + low * chan, full + high * chan), dz - 1, own)
                for dz in range(3)
            ],
            axis=0,
        )
        piece = lax.dot_general(left, right, NT, preferred_element_type=F32)
        for dz in range(3):
            for step in range(2):
                for dy in range(3):
                    at = base + step + dy - 1
                    if 0 <= at < height:
                        row = (dz * (high - low) + at - low) * chan
                        part = piece[row : row + chan, step * 4 * chan : (step + 1) * 4 * chan]
                        held = sums[dz][dy]
                        sums[dz][dy] = part if held is None else held + part
    if flip is not None:
        first = [jnp.where(flip, c, a) for a, c in zip(sums[0], sums[2])]
        third = [jnp.where(flip, a, c) for a, c in zip(sums[0], sums[2])]
        sums = [first, sums[1], third]
    for dz in range(2):
        for dy in range(3):
            row = (dz * 3 + dy) * chan
            out_ref[row : row + chan, : 3 * chan] = sums[dz][dy][:, : 3 * chan]
            out_ref[row : row + chan, 3 * chan :] = sums[2][dy][:, dz * chan : (dz + 1) * chan]
    for dy in range(3):
        out_ref[6 * chan :, dy * chan : (dy + 1) * chan] = sums[2][dy][:, 2 * chan : 3 * chan]
    out_ref[6 * chan :, 3 * chan :] = jnp.zeros((chan, chan), F32)


def main_kernel(count, sizes, *refs):
    chan, own, height, width, low_side, high_side = sizes
    full = chan * height
    mirrored = count == 2
    halos = low_side + high_side
    data_ref, cot_ref = refs[:2]
    halo_refs = refs[2 : 2 + halos]
    band_one, band_two, back_two = refs[2 + halos : 5 + halos]
    grad_field_ref, term_one, term_two = refs[5 + halos : 8 + halos]
    edge_ref, h_ref, g_ref, slope_ref, turn_ref = refs[8 + halos :]
    position = lax.axis_index("gz")
    flip = position == 1 if mirrored else None

    def reach(depth):
        return (-depth * low_side, own + depth * high_side)

    def field(ref, depth):
        before = depth if low_side else 1
        item = Field([(ref, -before, slots(sizes, depth), 0)], full, width)
        return blanked(item)

    def blanked(item):
        if not low_side:
            item.blank(-1)
        if not high_side:
            item.blank(own)
        return item

    def plane_of(ref, plane, skip, depth):
        if 0 <= plane < own:
            at = jnp.where(flip, own - 1 - plane, plane) if mirrored else plane
            return ref[:, at]
        if plane < 0:
            return halo_refs[0][:, skip + depth + plane]
        at = plane - own
        if mirrored:
            at = jnp.where(flip, depth - 1 - at, at)
        return halo_refs[-1][:, skip + at]

    def kept(plane, value):
        if count == 2:
            return value
        if plane < 0:
            return jnp.where(position > 0, value, 0.0)
        if plane >= own:
            return jnp.where(position < count - 1, value, 0.0)
        return value

    before = REACH if low_side else 1
    after = REACH if high_side else 1
    data = Field(
        [(data_ref, 0, own, 0), (edge_ref, -before, before, 0), (edge_ref, own, after, before)],
        full,
        width,
    )
    blanked(data)
    for plane in range(*reach(REACH)):
        if not 0 <= plane < own:
            data.put(plane, turned(turn_ref, plane % 2, plane_of(None, plane, 0, REACH)))

    hidden = field(h_ref, REACH - 1)
    slope_low, slope_high = reach(1)
    for first, number in spans(*reach(REACH - 1)):
        pre = data.convolve(band_one, first, number)
        for step in range(number):
            plane = first + step
            value = pre[:, step * width : (step + 1) * width]
            gate = sigmoid(value)
            hidden.put(plane, kept(plane, value * gate))
            if slope_low <= plane < slope_high:
                at = (plane - slope_low) * width
                slope_ref[:, at : at + width] = gate * (1.0 + value * (1.0 - gate))

    upper = field(g_ref, REACH - 2)
    for first, number in spans(*reach(REACH - 2)):
        pre = hidden.convolve(band_two, first, number)
        for step in range(number):
            plane = first + step
            value = pre[:, step * width : (step + 1) * width]
            gate = sigmoid(value)
            seed = turned(turn_ref, plane % 2, plane_of(cot_ref, plane, REACH, REACH - 2))
            upper.put(plane, seed * (gate * (1.0 + value * (1.0 - gate))))
    gradient(hidden, upper, own, chan, flip, term_two)

    lower = field(grad_field_ref, REACH - 3)
    for first, number in spans(*reach(REACH - 3)):
        back = upper.convolve(back_two, first, number)
        for step in range(number):
            plane = first + step
            at = (plane - slope_low) * width
            grad = back[:, step * width : (step + 1) * width] * slope_ref[:, at : at + width]
            lower.put(plane, kept(plane, grad))
    gradient(data, lower, own, chan, flip, term_one)


def slots(sizes, depth):
    _, own, _, _, low_side, high_side = sizes
    return own + sum(depth if side else 1 for side in (low_side, high_side))


def last_kernel(count, sizes, grad_field_ref, back_one, out_ref, turn_ref):
    chan, own, height, width, _, _ = sizes
    full = chan * height
    mirrored = count == 2
    flip = lax.axis_index("gz") == 1 if mirrored else None
    lower = Field([(grad_field_ref, -1, own + 2, 0)], full, width)
    for first, number in spans(0, own):
        out = lower.convolve(back_one, first, number)
        for step in range(number):
            plane = first + step
            value = out[:, step * width : (step + 1) * width]
            slot = plane % 2
            for y in range(height):
                turn_ref[slot, pl.ds(y, chan, stride=height), :] = value[y * chan : (y + 1) * chan]
            at = jnp.where(flip, own - 1 - plane, plane) if mirrored else plane
            out_ref[:, at] = turn_ref[slot].reshape(chan, height, width).astype(BF16)


def unpack_kernel(factor, one_ref, two_ref, out_one, out_two):
    chan = out_one.shape[-1]
    for ref, out in ((one_ref, out_one), (two_ref, out_two)):
        value = ref[...].T * factor
        for dz in range(3):
            for dy in range(3):
                for dx in range(3):
                    row, column = (dx, 3 * dz + dy) if dz < 2 else (3, 3 * dx + dy)
                    if dz == 2 and dx == 2:
                        row, column = dy, 6
                    out[dz, dy, dx] = value[
                        row * chan : (row + 1) * chan, column * chan : (column + 1) * chan
                    ]


def doubled(value, axis, before_last=None):
    count = lax.axis_size(axis)
    if count & (count - 1):
        value = before_last(value) if before_last else value
        return lax.psum(value, axis)
    step = 1
    while step < count:
        if before_last and step * 2 == count:
            value = before_last(value)
        value = value + lax.ppermute(value, axis, [(i, i ^ step) for i in range(count)])
        step *= 2
    return value


def reduced(one, two, grad_fields, finish):
    outs = []

    def gate(value):
        value, *held = lax.optimization_barrier((value, *grad_fields))
        outs.extend(finish(held))
        return value

    if lax.axis_size("gz") == 2:
        swap = [(0, 1), (1, 0)]
        first = lax.axis_index("gz") == 0
        mine = jnp.where(first, two, one)
        mine = mine + lax.ppermute(jnp.where(first, one, two), "gz", swap)
        mine = doubled(mine, "dp", gate)
        mine, *outs = lax.optimization_barrier((mine, *(outs or finish(grad_fields))))
        other = lax.ppermute(mine, "gz", swap)
        return jnp.where(first, other, mine), jnp.where(first, mine, other), outs
    both = doubled(doubled(jnp.stack([one, two]), "gz"), "dp", gate)
    return both[0], both[1], outs or finish(grad_fields)


def halo_of(data, cot, count):
    if count == 1:
        return []
    chan, own, height, width = data.shape
    sides = 1 if count == 2 else 2
    hbm = pl.BlockSpec(memory_space=pltpu.HBM)
    messages = pl.pallas_call(
        functools.partial(pack_kernel, count, own),
        out_shape=[jax.ShapeDtypeStruct((chan, 2 * REACH - 2, height, width), BF16)] * sides,
        in_specs=[hbm, hbm],
        scratch_shapes=[pltpu.SemaphoreType.DMA((sides, 2))],
        compiler_params=params(60),
        name="pack",
    )(data, cot)
    if count == 2:
        return [lax.ppermute(messages[0], "gz", [(0, 1), (1, 0)])]
    up = [(i, i + 1) for i in range(count - 1)]
    down = [(j, i) for i, j in up]
    return [lax.ppermute(messages[0], "gz", up), lax.ppermute(messages[1], "gz", down)]


def local(inputs, kernel_one, kernel_two, cotangent):
    count = lax.axis_size("gz")
    batch, chan, own, height, width = inputs.shape
    full = chan * height
    low_side, high_side = (1, 1) if count > 2 else (0, 1 if count == 2 else 0)
    sizes = (chan, own, height, width, low_side, high_side)
    taps = [jnp.transpose(k, (2, 3, 4, 0, 1)) for k in (kernel_one, kernel_two)]
    turn = pltpu.VMEM((2, full, width), F32)

    def stack(depth):
        return (3 * full, slots(sizes, depth) * width)

    grad_fields, backs, ones, twos = [], [], [], []
    for sample in range(batch):
        data, cot = inputs[sample], cotangent[sample]
        halos = halo_of(data, cot, count)
        *bands, field = pl.pallas_call(
            functools.partial(prep_kernel, count == 2),
            out_shape=[jax.ShapeDtypeStruct((3, full, 3 * full), BF16)] * 4
            + [jax.ShapeDtypeStruct((3 * full, own * width), BF16)],
            scratch_shapes=[pltpu.VMEM((3, 9 * chan, full), F32), turn],
            compiler_params=params(16),
            cost_estimate=cost(2e9, 5e6),
            name="prep",
        )(data, *taps)
        term = jax.ShapeDtypeStruct((7 * chan, 4 * chan), F32)
        grad_field, term_one, term_two = pl.pallas_call(
            functools.partial(main_kernel, count, sizes),
            out_shape=[jax.ShapeDtypeStruct(stack(REACH - 3), BF16), term, term],
            scratch_shapes=[
                pltpu.VMEM((3 * full, (slots(sizes, REACH) - own) * width), BF16),
                pltpu.VMEM(stack(REACH - 1), BF16),
                pltpu.VMEM(stack(REACH - 2), BF16),
                pltpu.VMEM((full, (own + low_side + high_side) * width), F32),
                turn,
            ],
            compiler_params=params(32),
            cost_estimate=cost(8e9, 8e6),
            name="main",
        )(field, cot, *halos, bands[0], bands[2], bands[3])
        grad_fields.append(grad_field)
        backs.append(bands[1])
        ones.append(term_one)
        twos.append(term_two)

    def finish(fields):
        return [
            pl.pallas_call(
                functools.partial(last_kernel, count, sizes),
                out_shape=jax.ShapeDtypeStruct((chan, own, height, width), BF16),
                scratch_shapes=[turn],
                compiler_params=params(16),
                cost_estimate=cost(2e9, 3e6),
                name="last",
            )(*pair)
            for pair in zip(fields, backs)
        ]

    one, two, outs = reduced(sum(ones[1:], ones[0]), sum(twos[1:], twos[0]), grad_fields, finish)
    cells = lax.axis_size("dp") * batch * count * own * height * width
    grads = pl.pallas_call(
        functools.partial(unpack_kernel, 1.0 / math.sqrt(cells)),
        out_shape=[jax.ShapeDtypeStruct((3, 3, 3, chan, chan), F32)] * 2,
        compiler_params=params(8),
        name="unpack",
    )(one, two)
    one, two = [jnp.transpose(g, (3, 4, 0, 1, 2)) for g in grads]
    return jnp.stack(outs), one, two


def solution(mesh):
    return jax.shard_map(
        local,
        mesh=mesh,
        in_specs=(P("dp", None, "gz", None, None), P(), P(), P("dp", None, "gz", None, None)),
        out_specs=(P("dp", None, "gz", None, None), P(), P()),
        check_vma=False,
    )
```

```python
import functools
import math

import jax
import jax.numpy as jnp
from jax import lax
from jax.experimental import pallas as pl
from jax.experimental.pallas import tpu as pltpu
from jax.sharding import PartitionSpec as P

F32, BF16 = jnp.float32, jnp.bfloat16
NT = (((1,), (1,)), ((), ()))
REACH = 4


def params(mib):
    return pltpu.CompilerParams(vmem_limit_bytes=mib * 2**20)


def cost(flops, size):
    return pl.CostEstimate(flops=int(flops), bytes_accessed=int(size), transcendentals=0)


def turned(turn_ref, slot, value):
    chan, height, width = value.shape
    turn_ref[slot] = value.astype(F32).reshape(chan * height, width)
    return jnp.concatenate(
        [turn_ref[slot, pl.ds(y, chan, stride=height), :] for y in range(height)], axis=0
    )


def prep_kernel(mirrored, data_ref, one_ref, two_ref, *refs):
    flip = lax.axis_index("gz") == 1 if mirrored else False
    outs, field_ref, wide, turn_ref = refs[:4], refs[4], refs[5], refs[6]
    chan = one_ref.shape[-1]
    full = outs[0].shape[1]
    height = full // chan
    own, width = data_ref.shape[1], data_ref.shape[-1]
    field = Field([(field_ref, 0, own, 0)], full, width)
    for plane in range(own):
        at = jnp.where(flip, own - 1 - plane, plane) if mirrored else plane
        field.put(plane, turned(turn_ref, plane % 2, data_ref[:, at]))
    lane = lax.broadcasted_iota(jnp.int32, (chan, full), 1)
    row = lax.broadcasted_iota(jnp.int32, (chan, full), 0)
    repeat = jnp.where(lax.rem(lane, chan) == row, 1.0, 0.0).astype(BF16)
    block = lane // chan
    for index, ref in enumerate((one_ref, two_ref)):
        forward, backward = outs[2 * index], outs[2 * index + 1]
        flat = ref[...].reshape(27 * chan, chan)
        spread = jnp.dot(flat, repeat, preferred_element_type=F32)
        wide[...] = spread.reshape(3, 9 * chan, full)
        for dz in range(3):
            source = jnp.where(flip, 2 - dz, dz) if mirrored else dz
            for dx in range(3):
                taps = [
                    wide[source, (dy * 3 + dx) * chan : (dy * 3 + dx + 1) * chan, :]
                    for dy in range(3)
                ]
                strips = []
                for y in range(height):
                    strip = jnp.zeros((chan, full), F32)
                    for dy in range(3):
                        strip = jnp.where(block == y + dy - 1, taps[dy], strip)
                    strips.append(strip.astype(BF16))
                tile = jnp.concatenate(strips, axis=0)
                forward[dz, :, dx * full : (dx + 1) * full] = tile
                backward[2 - dz, :, (2 - dx) * full : (3 - dx) * full] = tile.T


class Field:
    def __init__(self, pieces, full, width):
        self.pieces, self.full, self.width = pieces, full, width

    def run(self, plane, count):
        for ref, first, number, base in self.pieces:
            if first <= plane < first + number:
                at = plane - first
                size = min(count, number - at)
                return ref, slice((base + at) * self.width, (base + at + size) * self.width), size
        raise IndexError(plane)

    def take(self, rows, first, count):
        parts = []
        while count:
            ref, lanes, size = self.run(first, count)
            parts.append(ref[rows, lanes])
            first, count = first + size, count - size
        return parts[0] if len(parts) == 1 else jnp.concatenate(parts, axis=1)

    def put(self, plane, value):
        full, width = self.full, self.width
        ref, lanes, _ = self.run(plane, 1)
        lane = lax.broadcasted_iota(jnp.int32, (full, width), 1)
        before = jnp.where(lane == 0, 0.0, pltpu.roll(value, 1, 1))
        after = jnp.where(lane == width - 1, 0.0, pltpu.roll(value, width - 1, 1))
        for dx, item in enumerate((before, value, after)):
            ref[dx * full : (dx + 1) * full, lanes] = item.astype(BF16)

    def blank(self, plane):
        ref, lanes, _ = self.run(plane, 1)
        ref[:, lanes] = jnp.zeros((3 * self.full, self.width), BF16)

    def convolve(self, band, first, count):
        total = None
        for dz in range(3):
            window = self.take(slice(None), first + dz - 1, count)
            piece = jnp.dot(band[dz], window, preferred_element_type=F32)
            total = piece if total is None else total + piece
        return total


def spans(low, high):
    return [(at, min(2, high - at)) for at in range(low, high, 2)]


def sigmoid(value):
    return 0.5 * jnp.tanh(0.5 * value) + 0.5


def gradient(field, grads, own, chan, flip, out_ref):
    full = field.full
    height = full // chan
    sums = [[None] * 3 for _ in range(3)]
    for base in range(0, height, 2):
        right = jnp.concatenate(
            [
                grads.take(slice((2 - dx) * full + y * chan, (2 - dx) * full + (y + 1) * chan), 0, own)
                for y in (base, base + 1)
                for dx in (0, 1, 2, 2)
            ],
            axis=0,
        )
        low, high = max(base - 1, 0), min(base + 3, height)
        left = jnp.concatenate(
            [
                field.take(slice(full + low * chan, full + high * chan), dz - 1, own)
                for dz in range(3)
            ],
            axis=0,
        )
        piece = lax.dot_general(left, right, NT, preferred_element_type=F32)
        for dz in range(3):
            for step in range(2):
                for dy in range(3):
                    at = base + step + dy - 1
                    if 0 <= at < height:
                        row = (dz * (high - low) + at - low) * chan
                        part = piece[row : row + chan, step * 4 * chan : (step + 1) * 4 * chan]
                        held = sums[dz][dy]
                        sums[dz][dy] = part if held is None else held + part
    if flip is not None:
        first = [jnp.where(flip, c, a) for a, c in zip(sums[0], sums[2])]
        third = [jnp.where(flip, a, c) for a, c in zip(sums[0], sums[2])]
        sums = [first, sums[1], third]
    for dz in range(2):
        for dy in range(3):
            row = (dz * 3 + dy) * chan
            out_ref[row : row + chan, : 3 * chan] = sums[dz][dy][:, : 3 * chan]
            out_ref[row : row + chan, 3 * chan :] = sums[2][dy][:, dz * chan : (dz + 1) * chan]
    for dy in range(3):
        out_ref[6 * chan :, dy * chan : (dy + 1) * chan] = sums[2][dy][:, 2 * chan : 3 * chan]
    out_ref[6 * chan :, 3 * chan :] = jnp.zeros((chan, chan), F32)


def main_kernel(count, sizes, *refs):
    chan, own, height, width, low_side, high_side = sizes
    full = chan * height
    mirrored = count == 2
    halos = low_side + high_side
    data_ref, cot_ref = refs[:2]
    halo_refs = refs[2 : 2 + halos]
    band_one, band_two, back_two = refs[2 + halos : 5 + halos]
    grad_field_ref, term_one, term_two = refs[5 + halos : 8 + halos]
    edge_ref, h_ref, g_ref, slope_ref, turn_ref = refs[8 + halos :]
    position = lax.axis_index("gz")
    flip = position == 1 if mirrored else None

    def reach(depth):
        return (-depth * low_side, own + depth * high_side)

    def field(ref, depth):
        before = depth if low_side else 1
        item = Field([(ref, -before, slots(sizes, depth), 0)], full, width)
        return blanked(item)

    def blanked(item):
        if not low_side:
            item.blank(-1)
        if not high_side:
            item.blank(own)
        return item

    def plane_of(ref, plane, skip, depth):
        if 0 <= plane < own:
            at = jnp.where(flip, own - 1 - plane, plane) if mirrored else plane
            return ref[:, at]
        if plane < 0:
            return halo_refs[0][:, skip + depth + plane]
        at = plane - own
        if mirrored:
            at = jnp.where(flip, depth - 1 - at, at)
        return halo_refs[-1][:, skip + at]

    def kept(plane, value):
        if count == 2:
            return value
        if plane < 0:
            return jnp.where(position > 0, value, 0.0)
        if plane >= own:
            return jnp.where(position < count - 1, value, 0.0)
        return value

    before = REACH if low_side else 1
    after = REACH if high_side else 1
    data = Field(
        [(data_ref, 0, own, 0), (edge_ref, -before, before, 0), (edge_ref, own, after, before)],
        full,
        width,
    )
    blanked(data)
    for plane in range(*reach(REACH)):
        if not 0 <= plane < own:
            data.put(plane, turned(turn_ref, plane % 2, plane_of(None, plane, 0, REACH)))

    hidden = field(h_ref, REACH - 1)
    slope_low, slope_high = reach(1)
    for first, number in spans(*reach(REACH - 1)):
        pre = data.convolve(band_one, first, number)
        for step in range(number):
            plane = first + step
            value = pre[:, step * width : (step + 1) * width]
            gate = sigmoid(value)
            hidden.put(plane, kept(plane, value * gate))
            if slope_low <= plane < slope_high:
                at = (plane - slope_low) * width
                slope_ref[:, at : at + width] = gate * (1.0 + value * (1.0 - gate))

    upper = field(g_ref, REACH - 2)
    for first, number in spans(*reach(REACH - 2)):
        pre = hidden.convolve(band_two, first, number)
        for step in range(number):
            plane = first + step
            value = pre[:, step * width : (step + 1) * width]
            gate = sigmoid(value)
            seed = turned(turn_ref, plane % 2, plane_of(cot_ref, plane, REACH, REACH - 2))
            upper.put(plane, seed * (gate * (1.0 + value * (1.0 - gate))))
    gradient(hidden, upper, own, chan, flip, term_two)

    lower = field(grad_field_ref, REACH - 3)
    for first, number in spans(*reach(REACH - 3)):
        back = upper.convolve(back_two, first, number)
        for step in range(number):
            plane = first + step
            at = (plane - slope_low) * width
            grad = back[:, step * width : (step + 1) * width] * slope_ref[:, at : at + width]
            lower.put(plane, kept(plane, grad))
    gradient(data, lower, own, chan, flip, term_one)


def slots(sizes, depth):
    _, own, _, _, low_side, high_side = sizes
    return own + sum(depth if side else 1 for side in (low_side, high_side))


def last_kernel(count, sizes, grad_field_ref, back_one, out_ref, turn_ref):
    chan, own, height, width, _, _ = sizes
    full = chan * height
    mirrored = count == 2
    flip = lax.axis_index("gz") == 1 if mirrored else None
    lower = Field([(grad_field_ref, -1, own + 2, 0)], full, width)
    for first, number in spans(0, own):
        out = lower.convolve(back_one, first, number)
        for step in range(number):
            plane = first + step
            value = out[:, step * width : (step + 1) * width]
            slot = plane % 2
            for y in range(height):
                turn_ref[slot, pl.ds(y, chan, stride=height), :] = value[y * chan : (y + 1) * chan]
            at = jnp.where(flip, own - 1 - plane, plane) if mirrored else plane
            out_ref[:, at] = turn_ref[slot].reshape(chan, height, width).astype(BF16)


def unpack_kernel(factor, one_ref, two_ref, out_one, out_two):
    chan = out_one.shape[-1]
    for ref, out in ((one_ref, out_one), (two_ref, out_two)):
        value = ref[...].T * factor
        for dz in range(3):
            for dy in range(3):
                for dx in range(3):
                    row, column = (dx, 3 * dz + dy) if dz < 2 else (3, 3 * dx + dy)
                    if dz == 2 and dx == 2:
                        row, column = dy, 6
                    out[dz, dy, dx] = value[
                        row * chan : (row + 1) * chan, column * chan : (column + 1) * chan
                    ]


def doubled(value, axis):
    count = lax.axis_size(axis)
    if count & (count - 1):
        return lax.psum(value, axis)
    step = 1
    while step < count:
        value = value + lax.ppermute(value, axis, [(i, i ^ step) for i in range(count)])
        step *= 2
    return value


def crossed(value, before_last):
    count = lax.axis_size("dp")
    if count & (count - 1) or count == 1:
        return lax.psum(before_last(value), "dp")
    bits = [1 << k for k in range(count.bit_length() - 1)]
    groups = [bits[k : k + 2] for k in range(0, len(bits), 2)]
    partners = [group + [sum(group)] if len(group) == 2 else group for group in groups]
    turned_order = partners[::-1] if len(partners[-1]) == 3 else partners
    for phase, pair in enumerate(zip(partners, turned_order)):
        if phase == len(partners) - 1:
            value = before_last(value)
        sent = value.astype(BF16)
        parts = [sent]
        for steps in zip(*pair):
            moves = [
                (core * count + i, core * count + (i ^ step))
                for core, step in enumerate(steps)
                for i in range(count)
            ]
            parts.append(lax.ppermute(sent, ("gz", "dp"), moves))
        parts = [part.astype(F32) for part in parts]
        while len(parts) > 1:
            parts = [a + b for a, b in zip(parts[::2], parts[1::2])]
        value = parts[0]
    return value


def reduced(one, two, grad_fields, finish):
    outs = []

    def gate(value):
        value, *held = lax.optimization_barrier((value, *grad_fields))
        outs.extend(finish(held))
        return value

    if lax.axis_size("gz") == 2:
        swap = [(0, 1), (1, 0)]
        first = lax.axis_index("gz") == 0
        mine = jnp.where(first, two, one)
        mine = mine + lax.ppermute(jnp.where(first, one, two), "gz", swap)
        mine = crossed(mine, gate)
        mine, *outs = lax.optimization_barrier((mine, *outs))
        other = lax.ppermute(mine, "gz", swap)
        return jnp.where(first, other, mine), jnp.where(first, mine, other), outs
    both = doubled(doubled(jnp.stack([one, two]), "gz"), "dp")
    return both[0], both[1], finish(grad_fields)


def halo_of(data, cot, count):
    if count == 1:
        return []
    own = data.shape[1]

    def ends(low, high):
        flag = lax.axis_index("gz") == 1
        parts = []
        for value, depth in ((data, REACH), (cot, REACH - 2)):
            first, last = value[:, :depth], value[:, own - depth :]
            parts.append(jnp.where(flag, first, last) if low and high else first if low else last)
        return jnp.concatenate(parts, axis=1)

    if count == 2:
        return [lax.ppermute(ends(True, True), "gz", [(0, 1), (1, 0)])]
    up = [(i, i + 1) for i in range(count - 1)]
    down = [(j, i) for i, j in up]
    return [
        lax.ppermute(ends(False, True), "gz", up),
        lax.ppermute(ends(True, False), "gz", down),
    ]


def local(inputs, kernel_one, kernel_two, cotangent):
    count = lax.axis_size("gz")
    batch, chan, own, height, width = inputs.shape
    full = chan * height
    low_side, high_side = (1, 1) if count > 2 else (0, 1 if count == 2 else 0)
    sizes = (chan, own, height, width, low_side, high_side)
    taps = [jnp.transpose(k, (2, 3, 4, 0, 1)) for k in (kernel_one, kernel_two)]
    turn = pltpu.VMEM((2, full, width), F32)

    def stack(depth):
        return (3 * full, slots(sizes, depth) * width)

    grad_fields, backs, ones, twos = [], [], [], []
    for sample in range(batch):
        data, cot = inputs[sample], cotangent[sample]
        halos = halo_of(data, cot, count)
        *bands, field = pl.pallas_call(
            functools.partial(prep_kernel, count == 2),
            out_shape=[jax.ShapeDtypeStruct((3, full, 3 * full), BF16)] * 4
            + [jax.ShapeDtypeStruct((3 * full, own * width), BF16)],
            scratch_shapes=[pltpu.VMEM((3, 9 * chan, full), F32), turn],
            compiler_params=params(16),
            cost_estimate=cost(2e9, 5e6),
            name="prep",
        )(data, *taps)
        term = jax.ShapeDtypeStruct((7 * chan, 4 * chan), F32)
        grad_field, term_one, term_two = pl.pallas_call(
            functools.partial(main_kernel, count, sizes),
            out_shape=[jax.ShapeDtypeStruct(stack(REACH - 3), BF16), term, term],
            scratch_shapes=[
                pltpu.VMEM((3 * full, (slots(sizes, REACH) - own) * width), BF16),
                pltpu.VMEM(stack(REACH - 1), BF16),
                pltpu.VMEM(stack(REACH - 2), BF16),
                pltpu.VMEM((full, (own + low_side + high_side) * width), F32),
                turn,
            ],
            compiler_params=params(32),
            cost_estimate=cost(8e9, 8e6),
            name="main",
        )(field, cot, *halos, bands[0], bands[2], bands[3])
        grad_fields.append(grad_field)
        backs.append(bands[1])
        ones.append(term_one)
        twos.append(term_two)

    def finish(fields):
        return [
            pl.pallas_call(
                functools.partial(last_kernel, count, sizes),
                out_shape=jax.ShapeDtypeStruct((chan, own, height, width), BF16),
                scratch_shapes=[turn],
                compiler_params=params(16),
                cost_estimate=cost(2e9, 3e6),
                name="last",
            )(*pair)
            for pair in zip(fields, backs)
        ]

    one, two, outs = reduced(sum(ones[1:], ones[0]), sum(twos[1:], twos[0]), grad_fields, finish)
    cells = lax.axis_size("dp") * batch * count * own * height * width
    grads = pl.pallas_call(
        functools.partial(unpack_kernel, 1.0 / math.sqrt(cells)),
        out_shape=[jax.ShapeDtypeStruct((3, 3, 3, chan, chan), F32)] * 2,
        compiler_params=params(8),
        name="unpack",
    )(one, two)
    one, two = [jnp.transpose(g, (3, 4, 0, 1, 2)) for g in grads]
    return jnp.stack(outs), one, two


def solution(mesh):
    return jax.shard_map(
        local,
        mesh=mesh,
        in_specs=(P("dp", None, "gz", None, None), P(), P(), P("dp", None, "gz", None, None)),
        out_specs=(P("dp", None, "gz", None, None), P(), P()),
        check_vma=False,
    )
```

```python
import functools
import math

import jax
import jax.numpy as jnp
from jax import lax
from jax.experimental import pallas as pl
from jax.experimental.pallas import tpu as pltpu
from jax.sharding import PartitionSpec as P

F32, BF16 = jnp.float32, jnp.bfloat16
NT = (((1,), (1,)), ((), ()))
REACH = 4


def params(mib):
    return pltpu.CompilerParams(vmem_limit_bytes=mib * 2**20)


def cost(flops, size):
    return pl.CostEstimate(flops=int(flops), bytes_accessed=int(size), transcendentals=0)


def pack_kernel(count, own, *refs):
    sources, near, outs, sems = refs[:4], refs[4:8], refs[8:-1], refs[-1]
    pairs = []
    for side, out in enumerate(outs):
        for ref, depth, at in ((sources[0], REACH, 0), (sources[1], REACH - 2, REACH)):
            start = own - depth if side == 0 else 0
            if count == 2:
                start = jnp.where(lax.axis_index("gz") == 1, 0, own - depth)
            pairs.append((ref.at[:, pl.ds(start, depth)], out.at[:, pl.ds(at, depth)]))
    pairs.extend(zip(sources, near))
    copies = [pltpu.make_async_copy(*pair, sems.at[k]) for k, pair in enumerate(pairs)]
    for copy in copies:
        copy.start()
    for copy in copies:
        copy.wait()


def turned(turn_ref, slot, value):
    chan, height, width = value.shape
    turn_ref[slot] = value.astype(F32).reshape(chan * height, width)
    return jnp.concatenate(
        [turn_ref[slot, pl.ds(y, chan, stride=height), :] for y in range(height)], axis=0
    )


def layout(height):
    half = height // 2
    span = half + 1
    return half, span, (0, half - 1), -(-9 * span // 8) * 8


def prep_kernel(mirrored, data_ref, one_ref, two_ref, *refs):
    flip = lax.axis_index("gz") == 1 if mirrored else False
    outs, field_ref, wide_ref, turn_ref = refs[:4], refs[4], refs[5], refs[6]
    chan = one_ref.shape[-1]
    own, height, width = data_ref.shape[1:]
    full = chan * height
    field = Field([(field_ref, 0, own, 0)], full, width)
    for plane in range(own):
        at = jnp.where(flip, own - 1 - plane, plane) if mirrored else plane
        field.put(plane, turned(turn_ref, plane % 2, data_ref[:, at]))

    def iota(shape, dim):
        return lax.broadcasted_iota(jnp.int32, shape, dim)

    tile = 4 * chan
    same = lax.rem(iota((chan, tile), 1), chan) == iota((chan, tile), 0)
    repeat = jnp.where(same, 1.0, 0.0).astype(BF16)
    unit = jnp.where(iota((chan, chan), 0) == iota((chan, chan), 1), 1.0, 0.0).astype(BF16)
    row, lane = iota((tile, 4 * tile), 0), iota((tile, 4 * tile), 1)
    chosen = (row // chan == lane // tile) & (lax.rem(row, chan) == lax.rem(lane, chan))
    choose = jnp.where(chosen, 1.0, 0.0).astype(BF16)
    group = iota((chan, tile), 1) // chan
    half, span, lows, blocks = layout(height)
    for index, ref in enumerate((one_ref, two_ref)):
        flat = ref[...].reshape(27 * chan, chan)
        spread = jnp.dot(flat, repeat, preferred_element_type=F32)
        wide_ref[2 * index] = spread.reshape(3, 9 * chan, tile)
        flat = jnp.concatenate([flat, jnp.zeros((chan, chan), BF16)], axis=0)
        across = lax.dot_general(unit, flat, NT, preferred_element_type=F32).astype(BF16)
        stacked = jnp.concatenate([across[:, t * tile : (t + 1) * tile] for t in range(7)], axis=0)
        spread = jnp.dot(stacked, choose, preferred_element_type=F32)
        for tap in range(27):
            at, column = tap // 4 * chan, tap % 4 * tile
            wide_ref[2 * index + 1, tap // 9, tap % 9 * chan : (tap % 9 + 1) * chan] = spread[
                at : at + chan, column : column + tile
            ]
    for which, out in enumerate(outs):
        back = which % 2
        for part, low in enumerate(lows):
            for y in range(half):
                for first in range(0, blocks, 4):
                    strip = jnp.zeros((chan, tile), F32)
                    for block in range(first, min(first + 4, 9 * span)):
                        dz, dx = block // (3 * span), block // span % 3
                        dy = low + block % span - (part * half + y) + 1
                        if not 0 <= dy < 3:
                            continue
                        if back:
                            dz, dy, dx = 2 - dz, 2 - dy, 2 - dx
                        source = jnp.where(flip, 2 - dz, dz) if mirrored else dz
                        at = (dy * 3 + dx) * chan
                        tap = wide_ref[which, source, at : at + chan, :]
                        strip = jnp.where(group == block - first, tap, strip)
                    out[part, y * chan : (y + 1) * chan, first * chan : first * chan + tile] = (
                        strip.astype(BF16)
                    )


class Field:
    def __init__(self, pieces, full, width):
        self.pieces, self.full, self.width = pieces, full, width

    def run(self, plane, count):
        for ref, first, number, base in self.pieces:
            if first <= plane < first + number:
                at = plane - first
                size = min(count, number - at)
                return ref, slice((base + at) * self.width, (base + at + size) * self.width), size
        raise IndexError(plane)

    def take(self, rows, first, count):
        parts = []
        while count:
            ref, lanes, size = self.run(first, count)
            parts.append(ref[rows, lanes])
            first, count = first + size, count - size
        return parts[0] if len(parts) == 1 else jnp.concatenate(parts, axis=1)

    def put(self, plane, value):
        full, width = self.full, self.width
        ref, lanes, _ = self.run(plane, 1)
        lane = lax.broadcasted_iota(jnp.int32, (full, width), 1)
        before = jnp.where(lane == 0, 0.0, pltpu.roll(value, 1, 1))
        after = jnp.where(lane == width - 1, 0.0, pltpu.roll(value, width - 1, 1))
        for dx, item in enumerate((before, value, after)):
            ref[dx * full : (dx + 1) * full, lanes] = item.astype(BF16)

    def blank(self, plane):
        ref, lanes, _ = self.run(plane, 1)
        ref[:, lanes] = jnp.zeros((3 * self.full, self.width), BF16)

    def convolve(self, band, first, count, chan):
        half, span, lows, blocks = layout(self.full // chan)
        out = []
        for part, low in enumerate(lows):
            windows = [
                self.take(
                    slice(dx * self.full + low * chan, dx * self.full + (low + span) * chan),
                    first + dz - 1,
                    count,
                )
                for dz in range(3)
                for dx in range(3)
            ]
            if blocks > 9 * span:
                windows.append(self.take(slice(0, (blocks - 9 * span) * chan), first, count))
            window = jnp.concatenate(windows, axis=0)
            out.append(jnp.dot(band[part], window, preferred_element_type=F32))
        return jnp.concatenate(out, axis=0)


def spans(low, high):
    return [(at, min(2, high - at)) for at in range(low, high, 2)]


def sigmoid(value):
    return 0.5 * jnp.tanh(0.5 * value) + 0.5


def gradient(field, grads, own, chan, flip, out_ref):
    full = field.full
    height = full // chan
    sums = [[None] * 3 for _ in range(3)]
    for base in range(0, height, 2):
        right = jnp.concatenate(
            [
                grads.take(slice((2 - dx) * full + y * chan, (2 - dx) * full + (y + 1) * chan), 0, own)
                for y in (base, base + 1)
                for dx in (0, 1, 2, 2)
            ],
            axis=0,
        )
        low, high = max(base - 1, 0), min(base + 3, height)
        left = jnp.concatenate(
            [
                field.take(slice(full + low * chan, full + high * chan), dz - 1, own)
                for dz in range(3)
            ],
            axis=0,
        )
        piece = lax.dot_general(left, right, NT, preferred_element_type=F32)
        for dz in range(3):
            for step in range(2):
                for dy in range(3):
                    at = base + step + dy - 1
                    if 0 <= at < height:
                        row = (dz * (high - low) + at - low) * chan
                        part = piece[row : row + chan, step * 4 * chan : (step + 1) * 4 * chan]
                        held = sums[dz][dy]
                        sums[dz][dy] = part if held is None else held + part
    if flip is not None:
        first = [jnp.where(flip, c, a) for a, c in zip(sums[0], sums[2])]
        third = [jnp.where(flip, a, c) for a, c in zip(sums[0], sums[2])]
        sums = [first, sums[1], third]
    for dz in range(2):
        for dy in range(3):
            row = (dz * 3 + dy) * chan
            out_ref[row : row + chan, : 3 * chan] = sums[dz][dy][:, : 3 * chan]
            out_ref[row : row + chan, 3 * chan :] = sums[2][dy][:, dz * chan : (dz + 1) * chan]
    for dy in range(3):
        out_ref[6 * chan :, dy * chan : (dy + 1) * chan] = sums[2][dy][:, 2 * chan : 3 * chan]
    out_ref[6 * chan :, 3 * chan :] = jnp.zeros((chan, chan), F32)


def main_kernel(count, sizes, *refs):
    chan, own, height, width, low_side, high_side = sizes
    full = chan * height
    mirrored = count == 2
    halos = low_side + high_side
    data_ref, cot_ref = refs[:2]
    halo_refs = refs[2 : 2 + halos]
    band_one, band_two, back_two = refs[2 + halos : 5 + halos]
    grad_field_ref, term_one, term_two = refs[5 + halos : 8 + halos]
    edge_ref, h_ref, g_ref, slope_ref, turn_ref = refs[8 + halos :]
    position = lax.axis_index("gz")
    flip = position == 1 if mirrored else None

    def reach(depth):
        return (-depth * low_side, own + depth * high_side)

    def field(ref, depth):
        before = depth if low_side else 1
        item = Field([(ref, -before, slots(sizes, depth), 0)], full, width)
        return blanked(item)

    def blanked(item):
        if not low_side:
            item.blank(-1)
        if not high_side:
            item.blank(own)
        return item

    def plane_of(ref, plane, skip, depth):
        if 0 <= plane < own:
            at = jnp.where(flip, own - 1 - plane, plane) if mirrored else plane
            return ref[:, at]
        if plane < 0:
            return halo_refs[0][:, skip + depth + plane]
        at = plane - own
        if mirrored:
            at = jnp.where(flip, depth - 1 - at, at)
        return halo_refs[-1][:, skip + at]

    def kept(plane, value):
        if count == 2:
            return value
        if plane < 0:
            return jnp.where(position > 0, value, 0.0)
        if plane >= own:
            return jnp.where(position < count - 1, value, 0.0)
        return value

    before = REACH if low_side else 1
    after = REACH if high_side else 1
    data = Field(
        [(data_ref, 0, own, 0), (edge_ref, -before, before, 0), (edge_ref, own, after, before)],
        full,
        width,
    )
    blanked(data)
    for plane in range(*reach(REACH)):
        if not 0 <= plane < own:
            data.put(plane, turned(turn_ref, plane % 2, plane_of(None, plane, 0, REACH)))

    hidden = field(h_ref, REACH - 1)
    slope_low, slope_high = reach(1)
    for first, number in spans(*reach(REACH - 1)):
        pre = data.convolve(band_one, first, number, chan)
        for step in range(number):
            plane = first + step
            value = pre[:, step * width : (step + 1) * width]
            gate = sigmoid(value)
            hidden.put(plane, kept(plane, value * gate))
            if slope_low <= plane < slope_high:
                at = (plane - slope_low) * width
                slope_ref[:, at : at + width] = gate * (1.0 + value * (1.0 - gate))

    upper = field(g_ref, REACH - 2)
    for first, number in spans(*reach(REACH - 2)):
        pre = hidden.convolve(band_two, first, number, chan)
        for step in range(number):
            plane = first + step
            value = pre[:, step * width : (step + 1) * width]
            gate = sigmoid(value)
            seed = turned(turn_ref, plane % 2, plane_of(cot_ref, plane, REACH, REACH - 2))
            upper.put(plane, seed * (gate * (1.0 + value * (1.0 - gate))))
    gradient(hidden, upper, own, chan, flip, term_two)

    lower = field(grad_field_ref, REACH - 3)
    for first, number in spans(*reach(REACH - 3)):
        back = upper.convolve(back_two, first, number, chan)
        for step in range(number):
            plane = first + step
            at = (plane - slope_low) * width
            grad = back[:, step * width : (step + 1) * width] * slope_ref[:, at : at + width]
            lower.put(plane, kept(plane, grad))
    gradient(data, lower, own, chan, flip, term_one)


def slots(sizes, depth):
    _, own, _, _, low_side, high_side = sizes
    return own + sum(depth if side else 1 for side in (low_side, high_side))


def last_kernel(count, sizes, grad_field_ref, back_one, out_ref, turn_ref):
    chan, own, height, width, _, _ = sizes
    full = chan * height
    mirrored = count == 2
    flip = lax.axis_index("gz") == 1 if mirrored else None
    lower = Field([(grad_field_ref, -1, own + 2, 0)], full, width)
    for first, number in spans(0, own):
        out = lower.convolve(back_one, first, number, chan)
        for step in range(number):
            plane = first + step
            value = out[:, step * width : (step + 1) * width]
            slot = plane % 2
            for y in range(height):
                turn_ref[slot, pl.ds(y, chan, stride=height), :] = value[y * chan : (y + 1) * chan]
            at = jnp.where(flip, own - 1 - plane, plane) if mirrored else plane
            out_ref[:, at] = turn_ref[slot].reshape(chan, height, width).astype(BF16)


def unpack_kernel(factor, one_ref, two_ref, out_one, out_two):
    chan = out_one.shape[-1]
    for ref, out in ((one_ref, out_one), (two_ref, out_two)):
        value = ref[...].T * factor
        for dz in range(3):
            for dy in range(3):
                for dx in range(3):
                    row, column = (dx, 3 * dz + dy) if dz < 2 else (3, 3 * dx + dy)
                    if dz == 2 and dx == 2:
                        row, column = dy, 6
                    out[dz, dy, dx] = value[
                        row * chan : (row + 1) * chan, column * chan : (column + 1) * chan
                    ]


def doubled(value, axis):
    count = lax.axis_size(axis)
    if count & (count - 1):
        return lax.psum(value, axis)
    step = 1
    while step < count:
        value = value + lax.ppermute(value, axis, [(i, i ^ step) for i in range(count)])
        step *= 2
    return value


def crossed(value, before_last):
    count = lax.axis_size("dp")
    if count & (count - 1) or count == 1:
        return lax.psum(before_last(value), "dp")
    steps = [1 << k for k in range(count.bit_length() - 1)]
    half = len(steps) // 2
    other = steps[half:] + steps[:half]
    for phase, pair in enumerate(zip(other, steps)):
        if phase == len(steps) - 1:
            value = before_last(value)
        sent = value.astype(BF16)
        moves = [
            (core * count + i, core * count + (i ^ step))
            for core, step in enumerate(pair)
            for i in range(count)
        ]
        value = sent.astype(F32) + lax.ppermute(sent, ("gz", "dp"), moves).astype(F32)
    return value


def reduced(one, two, grad_fields, finish):
    outs = []

    def gate(value):
        value, *held = lax.optimization_barrier((value, *grad_fields))
        outs.extend(finish(held))
        return value

    if lax.axis_size("gz") == 2:
        swap = [(0, 1), (1, 0)]
        first = lax.axis_index("gz") == 0
        mine = jnp.where(first, two, one)
        mine = mine + lax.ppermute(jnp.where(first, one, two), "gz", swap)
        mine = crossed(mine, gate)
        mine, *outs = lax.optimization_barrier((mine, *outs))
        other = lax.ppermute(mine, "gz", swap)
        return jnp.where(first, other, mine), jnp.where(first, mine, other), outs
    both = doubled(doubled(jnp.stack([one, two]), "gz"), "dp")
    return both[0], both[1], finish(grad_fields)


def gathered(count, data, cot, *taps):
    chan, own, height, width = data.shape
    sides = min(count - 1, 2)
    arrays = (data, cot, *taps)
    far = [pltpu.with_memory_space_constraint(value, pltpu.HBM) for value in arrays]
    shapes = [value.shape for value in arrays]
    shapes += [(chan, 2 * REACH - 2, height, width)] * sides
    near = pl.pallas_call(
        functools.partial(pack_kernel, count, own),
        out_shape=[pltpu.VMEM(shape, BF16) for shape in shapes],
        in_specs=[pl.BlockSpec(memory_space=pltpu.HBM)] * 4,
        out_specs=[pl.BlockSpec(memory_space=pltpu.VMEM)] * len(shapes),
        scratch_shapes=[pltpu.SemaphoreType.DMA((4 + 2 * sides,))],
        compiler_params=params(4),
        name="pack",
    )(*far)
    messages = near[4:]
    if count == 2:
        moves = [[(0, 1), (1, 0)]]
    else:
        up = [(i, i + 1) for i in range(count - 1)]
        moves = [up, [(j, i) for i, j in up]]
    return near[:4], [lax.ppermute(item, "gz", move) for item, move in zip(messages, moves)]


def local(inputs, kernel_one, kernel_two, cotangent):
    count = lax.axis_size("gz")
    batch, chan, own, height, width = inputs.shape
    full = chan * height
    low_side, high_side = (1, 1) if count > 2 else (0, 1 if count == 2 else 0)
    sizes = (chan, own, height, width, low_side, high_side)
    taps = [jnp.transpose(k, (2, 3, 4, 0, 1)) for k in (kernel_one, kernel_two)]
    turn = pltpu.VMEM((2, full, width), F32)
    half, _, _, blocks = layout(height)

    def stack(depth):
        return (3 * full, slots(sizes, depth) * width)

    grad_fields, backs, ones, twos = [], [], [], []
    for sample in range(batch):
        near, halos = gathered(count, inputs[sample], cotangent[sample], *taps)
        data, cot, *near_taps = near
        *bands, field = pl.pallas_call(
            functools.partial(prep_kernel, count == 2),
            out_shape=[jax.ShapeDtypeStruct((2, half * chan, blocks * chan), BF16)] * 4
            + [jax.ShapeDtypeStruct((3 * full, own * width), BF16)],
            scratch_shapes=[pltpu.VMEM((4, 3, 9 * chan, 4 * chan), F32), turn],
            compiler_params=params(16),
            cost_estimate=cost(2e9, 5e6),
            name="prep",
        )(data, *near_taps)
        term = jax.ShapeDtypeStruct((7 * chan, 4 * chan), F32)
        grad_field, term_one, term_two = pl.pallas_call(
            functools.partial(main_kernel, count, sizes),
            out_shape=[jax.ShapeDtypeStruct(stack(REACH - 3), BF16), term, term],
            scratch_shapes=[
                pltpu.VMEM((3 * full, (slots(sizes, REACH) - own) * width), BF16),
                pltpu.VMEM(stack(REACH - 1), BF16),
                pltpu.VMEM(stack(REACH - 2), BF16),
                pltpu.VMEM((full, (own + low_side + high_side) * width), F32),
                turn,
            ],
            compiler_params=params(32),
            cost_estimate=cost(8e9, 8e6),
            name="main",
        )(field, cot, *halos, bands[0], bands[2], bands[3])
        grad_fields.append(grad_field)
        backs.append(bands[1])
        ones.append(term_one)
        twos.append(term_two)

    def finish(fields):
        return [
            pl.pallas_call(
                functools.partial(last_kernel, count, sizes),
                out_shape=jax.ShapeDtypeStruct((chan, own, height, width), BF16),
                scratch_shapes=[turn],
                compiler_params=params(16),
                cost_estimate=cost(2e9, 3e6),
                name="last",
            )(*pair)
            for pair in zip(fields, backs)
        ]

    one, two, outs = reduced(sum(ones[1:], ones[0]), sum(twos[1:], twos[0]), grad_fields, finish)
    cells = lax.axis_size("dp") * batch * count * own * height * width
    grads = pl.pallas_call(
        functools.partial(unpack_kernel, 1.0 / math.sqrt(cells)),
        out_shape=[jax.ShapeDtypeStruct((3, 3, 3, chan, chan), F32)] * 2,
        compiler_params=params(8),
        name="unpack",
    )(one, two)
    one, two = [jnp.transpose(g, (3, 4, 0, 1, 2)) for g in grads]
    return jnp.stack(outs), one, two


def solution(mesh):
    return jax.shard_map(
        local,
        mesh=mesh,
        in_specs=(P("dp", None, "gz", None, None), P(), P(), P("dp", None, "gz", None, None)),
        out_specs=(P("dp", None, "gz", None, None), P(), P()),
        check_vma=False,
    )
```

```python
import functools
import math

import jax
import jax.numpy as jnp
from jax import lax
from jax.experimental import pallas as pl
from jax.experimental.pallas import tpu as pltpu
from jax.sharding import PartitionSpec as P

F32, BF16 = jnp.float32, jnp.bfloat16
NT = (((1,), (1,)), ((), ()))
REACH = 4


def params(mib):
    return pltpu.CompilerParams(vmem_limit_bytes=mib * 2**20)


def cost(flops, size):
    return pl.CostEstimate(flops=int(flops), bytes_accessed=int(size), transcendentals=0)


def pack_kernel(count, own, *refs):
    sources, near, outs, sems = refs[:4], refs[4:8], refs[8:-1], refs[-1]
    pairs = []
    for side, out in enumerate(outs):
        for ref, depth, at in ((sources[0], REACH, 0), (sources[1], REACH - 2, REACH)):
            start = own - depth if side == 0 else 0
            if count == 2:
                start = jnp.where(lax.axis_index("gz") == 1, 0, own - depth)
            pairs.append((ref.at[:, pl.ds(start, depth)], out.at[:, pl.ds(at, depth)]))
    pairs.extend(zip(sources, near))
    copies = [pltpu.make_async_copy(*pair, sems.at[k]) for k, pair in enumerate(pairs)]
    for copy in copies:
        copy.start()
    for copy in copies:
        copy.wait()


def turned(turn_ref, slot, value):
    chan, height, width = value.shape
    turn_ref[slot] = value.astype(F32).reshape(chan * height, width)
    return jnp.concatenate(
        [turn_ref[slot, pl.ds(y, chan, stride=height), :] for y in range(height)], axis=0
    )


def layout(height):
    half = height // 2
    span = half + 1
    return half, span, (0, half - 1), -(-9 * span // 8) * 8


def prep_kernel(mirrored, data_ref, one_ref, two_ref, *refs):
    flip = lax.axis_index("gz") == 1 if mirrored else False
    outs, field_ref, wide_ref, turn_ref = refs[:4], refs[4], refs[5], refs[6]
    chan = one_ref.shape[-1]
    own, height, width = data_ref.shape[1:]
    full = chan * height
    field = Field([(field_ref, 0, own, 0)], full, width)
    for plane in range(own):
        at = jnp.where(flip, own - 1 - plane, plane) if mirrored else plane
        field.put(plane, turned(turn_ref, plane % 2, data_ref[:, at]))

    def iota(shape, dim):
        return lax.broadcasted_iota(jnp.int32, shape, dim)

    tile = 4 * chan
    same = lax.rem(iota((chan, tile), 1), chan) == iota((chan, tile), 0)
    repeat = jnp.where(same, 1.0, 0.0).astype(BF16)
    unit = jnp.where(iota((chan, chan), 0) == iota((chan, chan), 1), 1.0, 0.0).astype(BF16)
    row, lane = iota((tile, 4 * tile), 0), iota((tile, 4 * tile), 1)
    chosen = (row // chan == lane // tile) & (lax.rem(row, chan) == lax.rem(lane, chan))
    choose = jnp.where(chosen, 1.0, 0.0).astype(BF16)
    group = iota((chan, tile), 1) // chan
    half, span, lows, blocks = layout(height)
    for index, ref in enumerate((one_ref, two_ref)):
        flat = ref[...].reshape(27 * chan, chan)
        spread = jnp.dot(flat, repeat, preferred_element_type=F32)
        wide_ref[2 * index] = spread.reshape(3, 9 * chan, tile)
        flat = jnp.concatenate([flat, jnp.zeros((chan, chan), BF16)], axis=0)
        across = lax.dot_general(unit, flat, NT, preferred_element_type=F32).astype(BF16)
        stacked = jnp.concatenate([across[:, t * tile : (t + 1) * tile] for t in range(7)], axis=0)
        spread = jnp.dot(stacked, choose, preferred_element_type=F32)
        for tap in range(27):
            at, column = tap // 4 * chan, tap % 4 * tile
            wide_ref[2 * index + 1, tap // 9, tap % 9 * chan : (tap % 9 + 1) * chan] = spread[
                at : at + chan, column : column + tile
            ]
    for which, out in enumerate(outs):
        back = which % 2
        for part, low in enumerate(lows):
            for y in range(half):
                for first in range(0, blocks, 4):
                    strip = jnp.zeros((chan, tile), F32)
                    for block in range(first, min(first + 4, 9 * span)):
                        dz, dx = block // (3 * span), block // span % 3
                        dy = low + block % span - (part * half + y) + 1
                        if not 0 <= dy < 3:
                            continue
                        if back:
                            dz, dy, dx = 2 - dz, 2 - dy, 2 - dx
                        source = jnp.where(flip, 2 - dz, dz) if mirrored else dz
                        at = (dy * 3 + dx) * chan
                        tap = wide_ref[which, source, at : at + chan, :]
                        strip = jnp.where(group == block - first, tap, strip)
                    out[part, y * chan : (y + 1) * chan, first * chan : first * chan + tile] = (
                        strip.astype(BF16)
                    )


class Field:
    def __init__(self, pieces, full, width):
        self.pieces, self.full, self.width = pieces, full, width

    def run(self, plane, count):
        for ref, first, number, base in self.pieces:
            if first <= plane < first + number:
                at = plane - first
                size = min(count, number - at)
                return ref, slice((base + at) * self.width, (base + at + size) * self.width), size
        raise IndexError(plane)

    def take(self, rows, first, count):
        parts = []
        while count:
            ref, lanes, size = self.run(first, count)
            parts.append(ref[rows, lanes])
            first, count = first + size, count - size
        return parts[0] if len(parts) == 1 else jnp.concatenate(parts, axis=1)

    def put(self, plane, value):
        full, width = self.full, self.width
        ref, lanes, _ = self.run(plane, 1)
        lane = lax.broadcasted_iota(jnp.int32, (full, width), 1)
        before = jnp.where(lane == 0, 0.0, pltpu.roll(value, 1, 1))
        after = jnp.where(lane == width - 1, 0.0, pltpu.roll(value, width - 1, 1))
        for dx, item in enumerate((before, value, after)):
            ref[dx * full : (dx + 1) * full, lanes] = item.astype(BF16)

    def blank(self, plane):
        ref, lanes, _ = self.run(plane, 1)
        ref[:, lanes] = jnp.zeros((3 * self.full, self.width), BF16)

    def convolve(self, band, first, count, chan):
        half, span, lows, blocks = layout(self.full // chan)
        out = []
        for part, low in enumerate(lows):
            windows = [
                self.take(
                    slice(dx * self.full + low * chan, dx * self.full + (low + span) * chan),
                    first + dz - 1,
                    count,
                )
                for dz in range(3)
                for dx in range(3)
            ]
            if blocks > 9 * span:
                windows.append(self.take(slice(0, (blocks - 9 * span) * chan), first, count))
            window = jnp.concatenate(windows, axis=0)
            out.append(jnp.dot(band[part], window, preferred_element_type=F32))
        return jnp.concatenate(out, axis=0)


def spans(low, high):
    return [(at, min(2, high - at)) for at in range(low, high, 2)]


def sigmoid(value):
    return 0.5 * jnp.tanh(0.5 * value) + 0.5


def gradient(field, grads, own, chan, flip, out_ref):
    full = field.full
    height = full // chan
    sums = [[None] * 3 for _ in range(3)]
    for base in range(0, height, 2):
        right = jnp.concatenate(
            [
                grads.take(slice((2 - dx) * full + y * chan, (2 - dx) * full + (y + 1) * chan), 0, own)
                for y in (base, base + 1)
                for dx in (0, 1, 2, 2)
            ],
            axis=0,
        )
        low, high = max(base - 1, 0), min(base + 3, height)
        left = jnp.concatenate(
            [
                field.take(slice(full + low * chan, full + high * chan), dz - 1, own)
                for dz in range(3)
            ],
            axis=0,
        )
        piece = lax.dot_general(left, right, NT, preferred_element_type=F32)
        for dz in range(3):
            for step in range(2):
                for dy in range(3):
                    at = base + step + dy - 1
                    if 0 <= at < height:
                        row = (dz * (high - low) + at - low) * chan
                        part = piece[row : row + chan, step * 4 * chan : (step + 1) * 4 * chan]
                        held = sums[dz][dy]
                        sums[dz][dy] = part if held is None else held + part
    if flip is not None:
        first = [jnp.where(flip, c, a) for a, c in zip(sums[0], sums[2])]
        third = [jnp.where(flip, a, c) for a, c in zip(sums[0], sums[2])]
        sums = [first, sums[1], third]
    for dz in range(2):
        for dy in range(3):
            row = (dz * 3 + dy) * chan
            out_ref[row : row + chan, : 3 * chan] = sums[dz][dy][:, : 3 * chan]
            out_ref[row : row + chan, 3 * chan :] = sums[2][dy][:, dz * chan : (dz + 1) * chan]
    for dy in range(3):
        out_ref[6 * chan :, dy * chan : (dy + 1) * chan] = sums[2][dy][:, 2 * chan : 3 * chan]
    out_ref[6 * chan :, 3 * chan :] = jnp.zeros((chan, chan), F32)


def main_kernel(count, sizes, *refs):
    chan, own, height, width, low_side, high_side = sizes
    full = chan * height
    mirrored = count == 2
    halos = low_side + high_side
    data_ref, cot_ref = refs[:2]
    halo_refs = refs[2 : 2 + halos]
    band_one, band_two, back_two = refs[2 + halos : 5 + halos]
    grad_field_ref, term_one, term_two = refs[5 + halos : 8 + halos]
    edge_ref, h_ref, g_ref, slope_ref, turn_ref = refs[8 + halos :]
    position = lax.axis_index("gz")
    flip = position == 1 if mirrored else None

    def reach(depth):
        return (-depth * low_side, own + depth * high_side)

    def field(ref, depth):
        before = depth if low_side else 1
        item = Field([(ref, -before, slots(sizes, depth), 0)], full, width)
        return blanked(item)

    def blanked(item):
        if not low_side:
            item.blank(-1)
        if not high_side:
            item.blank(own)
        return item

    def plane_of(ref, plane, skip, depth):
        if 0 <= plane < own:
            at = jnp.where(flip, own - 1 - plane, plane) if mirrored else plane
            return ref[:, at]
        if plane < 0:
            return halo_refs[0][:, skip + depth + plane]
        at = plane - own
        if mirrored:
            at = jnp.where(flip, depth - 1 - at, at)
        return halo_refs[-1][:, skip + at]

    def kept(plane, value):
        if count == 2:
            return value
        if plane < 0:
            return jnp.where(position > 0, value, 0.0)
        if plane >= own:
            return jnp.where(position < count - 1, value, 0.0)
        return value

    before = REACH if low_side else 1
    after = REACH if high_side else 1
    data = Field(
        [(data_ref, 0, own, 0), (edge_ref, -before, before, 0), (edge_ref, own, after, before)],
        full,
        width,
    )
    blanked(data)
    for plane in range(*reach(REACH)):
        if not 0 <= plane < own:
            data.put(plane, turned(turn_ref, plane % 2, plane_of(None, plane, 0, REACH)))

    hidden = field(h_ref, REACH - 1)
    slope_low, slope_high = reach(1)
    for first, number in spans(*reach(REACH - 1)):
        pre = data.convolve(band_one, first, number, chan)
        for step in range(number):
            plane = first + step
            value = pre[:, step * width : (step + 1) * width]
            gate = sigmoid(value)
            hidden.put(plane, kept(plane, value * gate))
            if slope_low <= plane < slope_high:
                at = (plane - slope_low) * width
                slope_ref[:, at : at + width] = gate * (1.0 + value * (1.0 - gate))

    upper = field(g_ref, REACH - 2)
    for first, number in spans(*reach(REACH - 2)):
        pre = hidden.convolve(band_two, first, number, chan)
        for step in range(number):
            plane = first + step
            value = pre[:, step * width : (step + 1) * width]
            gate = sigmoid(value)
            seed = turned(turn_ref, plane % 2, plane_of(cot_ref, plane, REACH, REACH - 2))
            upper.put(plane, seed * (gate * (1.0 + value * (1.0 - gate))))
    gradient(hidden, upper, own, chan, flip, term_two)

    lower = field(grad_field_ref, REACH - 3)
    for first, number in spans(*reach(REACH - 3)):
        back = upper.convolve(back_two, first, number, chan)
        for step in range(number):
            plane = first + step
            at = (plane - slope_low) * width
            grad = back[:, step * width : (step + 1) * width] * slope_ref[:, at : at + width]
            lower.put(plane, kept(plane, grad))
    gradient(data, lower, own, chan, flip, term_one)


def slots(sizes, depth):
    _, own, _, _, low_side, high_side = sizes
    return own + sum(depth if side else 1 for side in (low_side, high_side))


def last_kernel(count, sizes, grad_field_ref, back_one, out_ref, turn_ref):
    chan, own, height, width, _, _ = sizes
    full = chan * height
    mirrored = count == 2
    flip = lax.axis_index("gz") == 1 if mirrored else None
    lower = Field([(grad_field_ref, -1, own + 2, 0)], full, width)
    for first, number in spans(0, own):
        out = lower.convolve(back_one, first, number, chan)
        for step in range(number):
            plane = first + step
            value = out[:, step * width : (step + 1) * width]
            slot = plane % 2
            for y in range(height):
                turn_ref[slot, pl.ds(y, chan, stride=height), :] = value[y * chan : (y + 1) * chan]
            at = jnp.where(flip, own - 1 - plane, plane) if mirrored else plane
            out_ref[:, at] = turn_ref[slot].reshape(chan, height, width).astype(BF16)


def unpack_kernel(factor, one_ref, two_ref, out_one, out_two):
    chan = out_one.shape[-1]
    for ref, out in ((one_ref, out_one), (two_ref, out_two)):
        value = ref[...].T * factor
        for dz in range(3):
            for dy in range(3):
                for dx in range(3):
                    row, column = (dx, 3 * dz + dy) if dz < 2 else (3, 3 * dx + dy)
                    if dz == 2 and dx == 2:
                        row, column = dy, 6
                    out[dz, dy, dx] = value[
                        row * chan : (row + 1) * chan, column * chan : (column + 1) * chan
                    ]


def doubled(value, axis):
    count = lax.axis_size(axis)
    if count & (count - 1):
        return lax.psum(value, axis)
    step = 1
    while step < count:
        value = value + lax.ppermute(value, axis, [(i, i ^ step) for i in range(count)])
        step *= 2
    return value


def odd(index):
    return bin(index).count("1") % 2


def crossed(value, before_last):
    count = lax.axis_size("dp")
    steps = [1 << k for k in range(count.bit_length() - 1)]
    half = len(steps) // 2
    orders = (steps[half:] + steps[:half], steps)
    for phase in range(len(steps)):
        if phase == len(steps) - 1:
            value = before_last(value)
        sent = value.astype(BF16)
        moves = []
        for core in range(2):
            for chip in range(count):
                step = orders[core ^ odd(chip)][phase]
                moves.append((core * count + chip, (1 - core) * count + (chip ^ step)))
        value = sent.astype(F32) + lax.ppermute(sent, ("gz", "dp"), moves).astype(F32)
    return value


def reduced(one, two, grad_fields, finish):
    outs = []

    def gate(value):
        value, *held = lax.optimization_barrier((value, *grad_fields))
        outs.extend(finish(held))
        return value

    count = lax.axis_size("dp")
    if lax.axis_size("gz") == 2 and count > 1 and count & (count - 1) == 0:
        swap = [(0, 1), (1, 0)]
        turns = lax.population_count(lax.axis_index("dp")) + lax.axis_index("gz")
        first = turns % 2 == 0
        mine = jnp.where(first, two, one)
        mine = mine + lax.ppermute(jnp.where(first, one, two), "gz", swap)
        mine = crossed(mine, gate)
        mine, *outs = lax.optimization_barrier((mine, *outs))
        other = lax.ppermute(mine, "gz", swap)
        return jnp.where(first, other, mine), jnp.where(first, mine, other), outs
    both = doubled(doubled(jnp.stack([one, two]), "gz"), "dp")
    return both[0], both[1], finish(grad_fields)


def gathered(count, data, cot, *taps):
    chan, own, height, width = data.shape
    sides = min(count - 1, 2)
    arrays = (data, cot, *taps)
    far = [pltpu.with_memory_space_constraint(value, pltpu.HBM) for value in arrays]
    shapes = [value.shape for value in arrays]
    shapes += [(chan, 2 * REACH - 2, height, width)] * sides
    near = pl.pallas_call(
        functools.partial(pack_kernel, count, own),
        out_shape=[pltpu.VMEM(shape, BF16) for shape in shapes],
        in_specs=[pl.BlockSpec(memory_space=pltpu.HBM)] * 4,
        out_specs=[pl.BlockSpec(memory_space=pltpu.VMEM)] * len(shapes),
        scratch_shapes=[pltpu.SemaphoreType.DMA((4 + 2 * sides,))],
        compiler_params=params(4),
        name="pack",
    )(*far)
    messages = near[4:]
    if count == 2:
        moves = [[(0, 1), (1, 0)]]
    else:
        up = [(i, i + 1) for i in range(count - 1)]
        moves = [up, [(j, i) for i, j in up]]
    return near[:4], [lax.ppermute(item, "gz", move) for item, move in zip(messages, moves)]


def local(inputs, kernel_one, kernel_two, cotangent):
    count = lax.axis_size("gz")
    batch, chan, own, height, width = inputs.shape
    full = chan * height
    low_side, high_side = (1, 1) if count > 2 else (0, 1 if count == 2 else 0)
    sizes = (chan, own, height, width, low_side, high_side)
    taps = [jnp.transpose(k, (2, 3, 4, 0, 1)) for k in (kernel_one, kernel_two)]
    turn = pltpu.VMEM((2, full, width), F32)
    half, _, _, blocks = layout(height)

    def stack(depth):
        return (3 * full, slots(sizes, depth) * width)

    grad_fields, backs, ones, twos = [], [], [], []
    for sample in range(batch):
        near, halos = gathered(count, inputs[sample], cotangent[sample], *taps)
        data, cot, *near_taps = near
        *bands, field = pl.pallas_call(
            functools.partial(prep_kernel, count == 2),
            out_shape=[jax.ShapeDtypeStruct((2, half * chan, blocks * chan), BF16)] * 4
            + [jax.ShapeDtypeStruct((3 * full, own * width), BF16)],
            scratch_shapes=[pltpu.VMEM((4, 3, 9 * chan, 4 * chan), F32), turn],
            compiler_params=params(16),
            cost_estimate=cost(2e9, 5e6),
            name="prep",
        )(data, *near_taps)
        term = jax.ShapeDtypeStruct((7 * chan, 4 * chan), F32)
        grad_field, term_one, term_two = pl.pallas_call(
            functools.partial(main_kernel, count, sizes),
            out_shape=[jax.ShapeDtypeStruct(stack(REACH - 3), BF16), term, term],
            scratch_shapes=[
                pltpu.VMEM((3 * full, (slots(sizes, REACH) - own) * width), BF16),
                pltpu.VMEM(stack(REACH - 1), BF16),
                pltpu.VMEM(stack(REACH - 2), BF16),
                pltpu.VMEM((full, (own + low_side + high_side) * width), F32),
                turn,
            ],
            compiler_params=params(32),
            cost_estimate=cost(8e9, 8e6),
            name="main",
        )(field, cot, *halos, bands[0], bands[2], bands[3])
        grad_fields.append(grad_field)
        backs.append(bands[1])
        ones.append(term_one)
        twos.append(term_two)

    def finish(fields):
        return [
            pl.pallas_call(
                functools.partial(last_kernel, count, sizes),
                out_shape=jax.ShapeDtypeStruct((chan, own, height, width), BF16),
                scratch_shapes=[turn],
                compiler_params=params(16),
                cost_estimate=cost(2e9, 3e6),
                name="last",
            )(*pair)
            for pair in zip(fields, backs)
        ]

    one, two, outs = reduced(sum(ones[1:], ones[0]), sum(twos[1:], twos[0]), grad_fields, finish)
    cells = lax.axis_size("dp") * batch * count * own * height * width
    grads = pl.pallas_call(
        functools.partial(unpack_kernel, 1.0 / math.sqrt(cells)),
        out_shape=[jax.ShapeDtypeStruct((3, 3, 3, chan, chan), F32)] * 2,
        compiler_params=params(8),
        name="unpack",
    )(one, two)
    one, two = [jnp.transpose(g, (3, 4, 0, 1, 2)) for g in grads]
    return jnp.stack(outs), one, two


def solution(mesh):
    return jax.shard_map(
        local,
        mesh=mesh,
        in_specs=(P("dp", None, "gz", None, None), P(), P(), P("dp", None, "gz", None, None)),
        out_specs=(P("dp", None, "gz", None, None), P(), P()),
        check_vma=False,
    )
```

```python
import functools
import math

import jax
import jax.numpy as jnp
from jax import lax
from jax.experimental import pallas as pl
from jax.experimental.pallas import tpu as pltpu
from jax.sharding import PartitionSpec as P

F32, BF16 = jnp.float32, jnp.bfloat16
NT = (((1,), (1,)), ((), ()))
REACH = 4


def params(mib):
    return pltpu.CompilerParams(vmem_limit_bytes=mib * 2**20)


def cost(flops, size):
    return pl.CostEstimate(flops=int(flops), bytes_accessed=int(size), transcendentals=0)


def pack_kernel(count, own, *refs):
    sources, near, outs, sems = refs[:4], refs[4:7], refs[7:-1], refs[-1]
    pairs = []
    for side, out in enumerate(outs):
        for ref, depth, at in ((sources[0], REACH, 0), (sources[1], REACH - 2, REACH)):
            start = own - depth if side == 0 else 0
            if count == 2:
                start = jnp.where(lax.axis_index("gz") == 1, 0, own - depth)
            pairs.append((ref.at[:, pl.ds(start, depth)], out.at[:, pl.ds(at, depth)]))
    pairs.extend(zip((sources[0], *sources[2:]), near))
    copies = [pltpu.make_async_copy(*pair, sems.at[k]) for k, pair in enumerate(pairs)]
    for copy in copies:
        copy.start()
    for copy in copies:
        copy.wait()


def turned(turn_ref, slot, value):
    chan, height, width = value.shape
    turn_ref[slot] = value.astype(F32).reshape(chan * height, width)
    return jnp.concatenate(
        [turn_ref[slot, pl.ds(y, chan, stride=height), :] for y in range(height)], axis=0
    )


def layout(height):
    half = height // 2
    span = half + 1
    return half, span, (0, half - 1), -(-9 * span // 8) * 8


def prep_kernel(mirrored, data_ref, one_ref, two_ref, *refs):
    flip = lax.axis_index("gz") == 1 if mirrored else False
    outs, field_ref, wide_ref, turn_ref = refs[:4], refs[4], refs[5], refs[6]
    chan = one_ref.shape[-1]
    own, height, width = data_ref.shape[1:]
    full = chan * height
    field = Field([(field_ref, 0, own, 0)], full, width)
    for plane in range(own):
        at = jnp.where(flip, own - 1 - plane, plane) if mirrored else plane
        field.put(plane, turned(turn_ref, plane % 2, data_ref[:, at]))

    def iota(shape, dim):
        return lax.broadcasted_iota(jnp.int32, shape, dim)

    tile = 4 * chan
    same = lax.rem(iota((chan, tile), 1), chan) == iota((chan, tile), 0)
    repeat = jnp.where(same, 1.0, 0.0).astype(BF16)
    unit = jnp.where(iota((chan, chan), 0) == iota((chan, chan), 1), 1.0, 0.0).astype(BF16)
    row, lane = iota((tile, 4 * tile), 0), iota((tile, 4 * tile), 1)
    chosen = (row // chan == lane // tile) & (lax.rem(row, chan) == lax.rem(lane, chan))
    choose = jnp.where(chosen, 1.0, 0.0).astype(BF16)
    group = iota((chan, tile), 1) // chan
    half, span, lows, blocks = layout(height)
    for index, ref in enumerate((one_ref, two_ref)):
        flat = ref[...].reshape(27 * chan, chan)
        spread = jnp.dot(flat, repeat, preferred_element_type=F32)
        wide_ref[2 * index] = spread.reshape(3, 9 * chan, tile)
        flat = jnp.concatenate([flat, jnp.zeros((chan, chan), BF16)], axis=0)
        across = lax.dot_general(unit, flat, NT, preferred_element_type=F32).astype(BF16)
        stacked = jnp.concatenate([across[:, t * tile : (t + 1) * tile] for t in range(7)], axis=0)
        spread = jnp.dot(stacked, choose, preferred_element_type=F32)
        for tap in range(27):
            at, column = tap // 4 * chan, tap % 4 * tile
            wide_ref[2 * index + 1, tap // 9, tap % 9 * chan : (tap % 9 + 1) * chan] = spread[
                at : at + chan, column : column + tile
            ]
    for which, out in enumerate(outs):
        back = which % 2
        for part, low in enumerate(lows):
            for y in range(half):
                for first in range(0, blocks, 4):
                    strip = jnp.zeros((chan, tile), F32)
                    for block in range(first, min(first + 4, 9 * span)):
                        dz, dx = block // (3 * span), block // span % 3
                        dy = low + block % span - (part * half + y) + 1
                        if not 0 <= dy < 3:
                            continue
                        if back:
                            dz, dy, dx = 2 - dz, 2 - dy, 2 - dx
                        source = jnp.where(flip, 2 - dz, dz) if mirrored else dz
                        at = (dy * 3 + dx) * chan
                        tap = wide_ref[which, source, at : at + chan, :]
                        strip = jnp.where(group == block - first, tap, strip)
                    out[part, y * chan : (y + 1) * chan, first * chan : first * chan + tile] = (
                        strip.astype(BF16)
                    )


class Field:
    def __init__(self, pieces, full, width):
        self.pieces, self.full, self.width = pieces, full, width

    def run(self, plane, count):
        for ref, first, number, base in self.pieces:
            if first <= plane < first + number:
                at = plane - first
                size = min(count, number - at)
                return ref, slice((base + at) * self.width, (base + at + size) * self.width), size
        raise IndexError(plane)

    def take(self, rows, first, count):
        parts = []
        while count:
            ref, lanes, size = self.run(first, count)
            parts.append(ref[rows, lanes])
            first, count = first + size, count - size
        return parts[0] if len(parts) == 1 else jnp.concatenate(parts, axis=1)

    def put(self, plane, value):
        full, width = self.full, self.width
        ref, lanes, _ = self.run(plane, 1)
        lane = lax.broadcasted_iota(jnp.int32, (full, width), 1)
        before = jnp.where(lane == 0, 0.0, pltpu.roll(value, 1, 1))
        after = jnp.where(lane == width - 1, 0.0, pltpu.roll(value, width - 1, 1))
        for dx, item in enumerate((before, value, after)):
            ref[dx * full : (dx + 1) * full, lanes] = item.astype(BF16)

    def blank(self, plane):
        ref, lanes, _ = self.run(plane, 1)
        ref[:, lanes] = jnp.zeros((3 * self.full, self.width), BF16)

    def convolve(self, band, first, count, chan):
        half, span, lows, blocks = layout(self.full // chan)
        out = []
        for part, low in enumerate(lows):
            windows = [
                self.take(
                    slice(dx * self.full + low * chan, dx * self.full + (low + span) * chan),
                    first + dz - 1,
                    count,
                )
                for dz in range(3)
                for dx in range(3)
            ]
            if blocks > 9 * span:
                windows.append(self.take(slice(0, (blocks - 9 * span) * chan), first, count))
            window = jnp.concatenate(windows, axis=0)
            out.append(jnp.dot(band[part], window, preferred_element_type=F32))
        return jnp.concatenate(out, axis=0)


def spans(low, high):
    return [(at, min(2, high - at)) for at in range(low, high, 2)]


def sigmoid(value):
    return 0.5 * jnp.tanh(0.5 * value) + 0.5


def gradient(field, grads, own, chan, flip, out_ref):
    full = field.full
    height = full // chan
    sums = [[None] * 3 for _ in range(3)]
    for base in range(0, height, 2):
        right = jnp.concatenate(
            [
                grads.take(slice((2 - dx) * full + y * chan, (2 - dx) * full + (y + 1) * chan), 0, own)
                for y in (base, base + 1)
                for dx in (0, 1, 2, 2)
            ],
            axis=0,
        )
        low, high = max(base - 1, 0), min(base + 3, height)
        left = jnp.concatenate(
            [
                field.take(slice(full + low * chan, full + high * chan), dz - 1, own)
                for dz in range(3)
            ],
            axis=0,
        )
        piece = lax.dot_general(left, right, NT, preferred_element_type=F32)
        for dz in range(3):
            for step in range(2):
                for dy in range(3):
                    at = base + step + dy - 1
                    if 0 <= at < height:
                        row = (dz * (high - low) + at - low) * chan
                        part = piece[row : row + chan, step * 4 * chan : (step + 1) * 4 * chan]
                        held = sums[dz][dy]
                        sums[dz][dy] = part if held is None else held + part
    if flip is not None:
        first = [jnp.where(flip, c, a) for a, c in zip(sums[0], sums[2])]
        third = [jnp.where(flip, a, c) for a, c in zip(sums[0], sums[2])]
        sums = [first, sums[1], third]
    for dz in range(2):
        for dy in range(3):
            row = (dz * 3 + dy) * chan
            out_ref[row : row + chan, : 3 * chan] = sums[dz][dy][:, : 3 * chan]
            out_ref[row : row + chan, 3 * chan :] = sums[2][dy][:, dz * chan : (dz + 1) * chan]
    for dy in range(3):
        out_ref[6 * chan :, dy * chan : (dy + 1) * chan] = sums[2][dy][:, 2 * chan : 3 * chan]
    out_ref[6 * chan :, 3 * chan :] = jnp.zeros((chan, chan), F32)


def main_kernel(count, sizes, *refs):
    chan, own, height, width, low_side, high_side = sizes
    full = chan * height
    mirrored = count == 2
    halos = low_side + high_side
    data_ref, cot_ref = refs[:2]
    halo_refs = refs[2 : 2 + halos]
    band_one, band_two, back_two = refs[2 + halos : 5 + halos]
    grad_field_ref, term_one, term_two = refs[5 + halos : 8 + halos]
    edge_ref, h_ref, g_ref, slope_ref, turn_ref = refs[8 + halos :]
    position = lax.axis_index("gz")
    flip = position == 1 if mirrored else None

    def reach(depth):
        return (-depth * low_side, own + depth * high_side)

    def field(ref, depth):
        before = depth if low_side else 1
        item = Field([(ref, -before, slots(sizes, depth), 0)], full, width)
        return blanked(item)

    def blanked(item):
        if not low_side:
            item.blank(-1)
        if not high_side:
            item.blank(own)
        return item

    def plane_of(ref, plane, skip, depth):
        if 0 <= plane < own:
            at = jnp.where(flip, own - 1 - plane, plane) if mirrored else plane
            return ref[:, at]
        if plane < 0:
            return halo_refs[0][:, skip + depth + plane]
        at = plane - own
        if mirrored:
            at = jnp.where(flip, depth - 1 - at, at)
        return halo_refs[-1][:, skip + at]

    def kept(plane, value):
        if count == 2:
            return value
        if plane < 0:
            return jnp.where(position > 0, value, 0.0)
        if plane >= own:
            return jnp.where(position < count - 1, value, 0.0)
        return value

    before = REACH if low_side else 1
    after = REACH if high_side else 1
    data = Field(
        [(data_ref, 0, own, 0), (edge_ref, -before, before, 0), (edge_ref, own, after, before)],
        full,
        width,
    )
    blanked(data)
    for plane in range(*reach(REACH)):
        if not 0 <= plane < own:
            data.put(plane, turned(turn_ref, plane % 2, plane_of(None, plane, 0, REACH)))

    hidden = field(h_ref, REACH - 1)
    slope_low, slope_high = reach(1)
    for first, number in spans(*reach(REACH - 1)):
        pre = data.convolve(band_one, first, number, chan)
        for step in range(number):
            plane = first + step
            value = pre[:, step * width : (step + 1) * width]
            gate = sigmoid(value)
            hidden.put(plane, kept(plane, value * gate))
            if slope_low <= plane < slope_high:
                at = (plane - slope_low) * width
                slope_ref[:, at : at + width] = gate * (1.0 + value * (1.0 - gate))

    upper = field(g_ref, REACH - 2)
    for first, number in spans(*reach(REACH - 2)):
        pre = hidden.convolve(band_two, first, number, chan)
        for step in range(number):
            plane = first + step
            value = pre[:, step * width : (step + 1) * width]
            gate = sigmoid(value)
            seed = turned(turn_ref, plane % 2, plane_of(cot_ref, plane, REACH, REACH - 2))
            upper.put(plane, seed * (gate * (1.0 + value * (1.0 - gate))))

    lower = field(grad_field_ref, REACH - 3)
    for first, number in spans(*reach(REACH - 3)):
        back = upper.convolve(back_two, first, number, chan)
        for step in range(number):
            plane = first + step
            at = (plane - slope_low) * width
            grad = back[:, step * width : (step + 1) * width] * slope_ref[:, at : at + width]
            lower.put(plane, kept(plane, grad))
    gradient(hidden, upper, own, chan, flip, term_two)
    gradient(data, lower, own, chan, flip, term_one)


def slots(sizes, depth):
    _, own, _, _, low_side, high_side = sizes
    return own + sum(depth if side else 1 for side in (low_side, high_side))


def last_kernel(count, sizes, grad_field_ref, back_one, out_ref, turn_ref):
    chan, own, height, width, _, _ = sizes
    full = chan * height
    mirrored = count == 2
    flip = lax.axis_index("gz") == 1 if mirrored else None
    lower = Field([(grad_field_ref, -1, own + 2, 0)], full, width)
    for first, number in spans(0, own):
        out = lower.convolve(back_one, first, number, chan)
        for step in range(number):
            plane = first + step
            value = out[:, step * width : (step + 1) * width]
            slot = plane % 2
            for y in range(height):
                turn_ref[slot, pl.ds(y, chan, stride=height), :] = value[y * chan : (y + 1) * chan]
            at = jnp.where(flip, own - 1 - plane, plane) if mirrored else plane
            out_ref[:, at] = turn_ref[slot].reshape(chan, height, width).astype(BF16)


def unpack_kernel(factor, one_ref, two_ref, out_one, out_two):
    chan = out_one.shape[-1]
    for ref, out in ((one_ref, out_one), (two_ref, out_two)):
        value = ref[...].T * factor
        for dz in range(3):
            for dy in range(3):
                for dx in range(3):
                    row, column = (dx, 3 * dz + dy) if dz < 2 else (3, 3 * dx + dy)
                    if dz == 2 and dx == 2:
                        row, column = dy, 6
                    out[dz, dy, dx] = value[
                        row * chan : (row + 1) * chan, column * chan : (column + 1) * chan
                    ]


def doubled(value, axis):
    count = lax.axis_size(axis)
    if count & (count - 1):
        return lax.psum(value, axis)
    step = 1
    while step < count:
        value = value + lax.ppermute(value, axis, [(i, i ^ step) for i in range(count)])
        step *= 2
    return value


def odd(index):
    return bin(index).count("1") % 2


def crossed(value, before_last):
    count = lax.axis_size("dp")
    steps = [1 << k for k in range(count.bit_length() - 1)]
    near, far = steps[:-1], steps[-1:]
    orders = (near[:1] + far + near[1:], near[-1:] + near[:1] + far + near[1:-1])
    if len(steps) < 3:
        orders = (steps, steps)
    for phase in range(len(steps)):
        if phase == len(steps) - 1:
            value = before_last(value)
        sent = value.astype(BF16)
        moves = []
        for core in range(2):
            for chip in range(count):
                step = orders[core ^ odd(chip)][phase]
                moves.append((core * count + chip, (1 - core) * count + (chip ^ step)))
        value = sent.astype(F32) + lax.ppermute(sent, ("gz", "dp"), moves).astype(F32)
    return value


def reduced(one, two, grad_fields, finish):
    outs = []

    def gate(value):
        value, *held = lax.optimization_barrier((value, *grad_fields))
        outs.extend(finish(held))
        return value

    count = lax.axis_size("dp")
    if lax.axis_size("gz") == 2 and count > 1 and count & (count - 1) == 0:
        swap = [(0, 1), (1, 0)]
        turns = lax.population_count(lax.axis_index("dp")) + lax.axis_index("gz")
        first = turns % 2 == 0
        mine = jnp.where(first, two, one)
        mine = mine + lax.ppermute(jnp.where(first, one, two), "gz", swap)
        mine = crossed(mine, gate)
        mine, *outs = lax.optimization_barrier((mine, *outs))
        other = lax.ppermute(mine, "gz", swap)
        return jnp.where(first, other, mine), jnp.where(first, mine, other), outs
    both = doubled(doubled(jnp.stack([one, two]), "gz"), "dp")
    return both[0], both[1], finish(grad_fields)


def gathered(count, data, cot, *taps):
    chan, own, height, width = data.shape
    sides = min(count - 1, 2)
    arrays = (data, cot, *taps)
    far = [pltpu.with_memory_space_constraint(value, pltpu.HBM) for value in arrays]
    shapes = [value.shape for value in (data, *taps)]
    shapes += [(chan, 2 * REACH - 2, height, width)] * sides
    near = pl.pallas_call(
        functools.partial(pack_kernel, count, own),
        out_shape=[pltpu.VMEM(shape, BF16) for shape in shapes],
        in_specs=[pl.BlockSpec(memory_space=pltpu.HBM)] * 4,
        out_specs=[pl.BlockSpec(memory_space=pltpu.VMEM)] * len(shapes),
        scratch_shapes=[pltpu.SemaphoreType.DMA((3 + 2 * sides,))],
        compiler_params=params(4),
        name="pack",
    )(*far)
    messages = near[3:]
    if count == 2:
        moves = [[(0, 1), (1, 0)]]
    else:
        up = [(i, i + 1) for i in range(count - 1)]
        moves = [up, [(j, i) for i, j in up]]
    return [near[0], cot, *near[1:3]], [lax.ppermute(item, "gz", move) for item, move in zip(messages, moves)]


def local(inputs, kernel_one, kernel_two, cotangent):
    count = lax.axis_size("gz")
    batch, chan, own, height, width = inputs.shape
    full = chan * height
    low_side, high_side = (1, 1) if count > 2 else (0, 1 if count == 2 else 0)
    sizes = (chan, own, height, width, low_side, high_side)
    taps = [jnp.transpose(k, (2, 3, 4, 0, 1)) for k in (kernel_one, kernel_two)]
    turn = pltpu.VMEM((2, full, width), F32)
    half, _, _, blocks = layout(height)

    def stack(depth):
        return (3 * full, slots(sizes, depth) * width)

    grad_fields, backs, ones, twos = [], [], [], []
    for sample in range(batch):
        near, halos = gathered(count, inputs[sample], cotangent[sample], *taps)
        data, cot, *near_taps = near
        *bands, field = pl.pallas_call(
            functools.partial(prep_kernel, count == 2),
            out_shape=[jax.ShapeDtypeStruct((2, half * chan, blocks * chan), BF16)] * 4
            + [jax.ShapeDtypeStruct((3 * full, own * width), BF16)],
            scratch_shapes=[pltpu.VMEM((4, 3, 9 * chan, 4 * chan), F32), turn],
            compiler_params=params(16),
            cost_estimate=cost(2e9, 5e6),
            name="prep",
        )(data, *near_taps)
        term = jax.ShapeDtypeStruct((7 * chan, 4 * chan), F32)
        grad_field, term_one, term_two = pl.pallas_call(
            functools.partial(main_kernel, count, sizes),
            out_shape=[jax.ShapeDtypeStruct(stack(REACH - 3), BF16), term, term],
            scratch_shapes=[
                pltpu.VMEM((3 * full, (slots(sizes, REACH) - own) * width), BF16),
                pltpu.VMEM(stack(REACH - 1), BF16),
                pltpu.VMEM(stack(REACH - 2), BF16),
                pltpu.VMEM((full, (own + low_side + high_side) * width), F32),
                turn,
            ],
            compiler_params=params(32),
            cost_estimate=cost(8e9, 8e6),
            name="main",
        )(field, cot, *halos, bands[0], bands[2], bands[3])
        grad_fields.append(grad_field)
        backs.append(bands[1])
        ones.append(term_one)
        twos.append(term_two)

    def finish(fields):
        return [
            pl.pallas_call(
                functools.partial(last_kernel, count, sizes),
                out_shape=jax.ShapeDtypeStruct((chan, own, height, width), BF16),
                scratch_shapes=[turn],
                compiler_params=params(16),
                cost_estimate=cost(2e9, 3e6),
                name="last",
            )(*pair)
            for pair in zip(fields, backs)
        ]

    one, two, outs = reduced(sum(ones[1:], ones[0]), sum(twos[1:], twos[0]), grad_fields, finish)
    cells = lax.axis_size("dp") * batch * count * own * height * width
    grads = pl.pallas_call(
        functools.partial(unpack_kernel, 1.0 / math.sqrt(cells)),
        out_shape=[jax.ShapeDtypeStruct((3, 3, 3, chan, chan), F32)] * 2,
        compiler_params=params(8),
        name="unpack",
    )(one, two)
    one, two = [jnp.transpose(g, (3, 4, 0, 1, 2)) for g in grads]
    return jnp.stack(outs), one, two


def solution(mesh):
    return jax.shard_map(
        local,
        mesh=mesh,
        in_specs=(P("dp", None, "gz", None, None), P(), P(), P("dp", None, "gz", None, None)),
        out_specs=(P("dp", None, "gz", None, None), P(), P()),
        check_vma=False,
    )
```

```python
import functools
import math

import jax
import jax.numpy as jnp
from jax import lax
from jax.experimental import pallas as pl
from jax.experimental.pallas import tpu as pltpu
from jax.sharding import PartitionSpec as P

F32, BF16 = jnp.float32, jnp.bfloat16
NT = (((1,), (1,)), ((), ()))
REACH = 4


def params(mib):
    return pltpu.CompilerParams(vmem_limit_bytes=mib * 2**20)


def cost(flops, size):
    return pl.CostEstimate(flops=int(flops), bytes_accessed=int(size), transcendentals=0)


def pack_kernel(count, own, *refs):
    sources, near, outs, sems = refs[:4], refs[4:7], refs[7:-1], refs[-1]
    pairs = []
    for side, out in enumerate(outs):
        for ref, depth, at in ((sources[0], REACH, 0), (sources[1], REACH - 2, REACH)):
            start = own - depth if side == 0 else 0
            if count == 2:
                start = jnp.where(lax.axis_index("gz") == 1, 0, own - depth)
            pairs.append((ref.at[:, pl.ds(start, depth)], out.at[:, pl.ds(at, depth)]))
    pairs.extend(zip((sources[0], *sources[2:]), near))
    copies = [pltpu.make_async_copy(*pair, sems.at[k]) for k, pair in enumerate(pairs)]
    for copy in copies:
        copy.start()
    for copy in copies:
        copy.wait()


def turned(turn_ref, slot, value):
    chan, height, width = value.shape
    turn_ref[slot] = value.astype(F32).reshape(chan * height, width)
    return jnp.concatenate(
        [turn_ref[slot, pl.ds(y, chan, stride=height), :] for y in range(height)], axis=0
    )


def layout(height):
    half = height // 2
    span = half + 1
    return half, span, (0, half - 1), -(-9 * span // 8) * 8


def prep_kernel(mirrored, data_ref, one_ref, two_ref, *refs):
    flip = lax.axis_index("gz") == 1 if mirrored else False
    outs, field_ref, wide_ref, turn_ref = refs[:4], refs[4], refs[5], refs[6]
    chan = one_ref.shape[-1]
    own, height, width = data_ref.shape[1:]
    full = chan * height
    field = Field([(field_ref, 0, own, 0)], full, width)
    for plane in range(own):
        at = jnp.where(flip, own - 1 - plane, plane) if mirrored else plane
        field.put(plane, turned(turn_ref, plane % 2, data_ref[:, at]))

    def iota(shape, dim):
        return lax.broadcasted_iota(jnp.int32, shape, dim)

    tile = 4 * chan
    same = lax.rem(iota((chan, tile), 1), chan) == iota((chan, tile), 0)
    repeat = jnp.where(same, 1.0, 0.0).astype(BF16)
    unit = jnp.where(iota((chan, chan), 0) == iota((chan, chan), 1), 1.0, 0.0).astype(BF16)
    row, lane = iota((tile, 4 * tile), 0), iota((tile, 4 * tile), 1)
    chosen = (row // chan == lane // tile) & (lax.rem(row, chan) == lax.rem(lane, chan))
    choose = jnp.where(chosen, 1.0, 0.0).astype(BF16)
    group = iota((chan, tile), 1) // chan
    half, span, lows, blocks = layout(height)
    for index, ref in enumerate((one_ref, two_ref)):
        flat = ref[...].reshape(27 * chan, chan)
        spread = jnp.dot(flat, repeat, preferred_element_type=F32)
        wide_ref[2 * index] = spread.reshape(3, 9 * chan, tile)
        flat = jnp.concatenate([flat, jnp.zeros((chan, chan), BF16)], axis=0)
        across = lax.dot_general(unit, flat, NT, preferred_element_type=F32).astype(BF16)
        stacked = jnp.concatenate([across[:, t * tile : (t + 1) * tile] for t in range(7)], axis=0)
        spread = jnp.dot(stacked, choose, preferred_element_type=F32)
        for tap in range(27):
            at, column = tap // 4 * chan, tap % 4 * tile
            wide_ref[2 * index + 1, tap // 9, tap % 9 * chan : (tap % 9 + 1) * chan] = spread[
                at : at + chan, column : column + tile
            ]
    for which, out in enumerate(outs):
        back = which % 2
        for part, low in enumerate(lows):
            for y in range(half):
                for first in range(0, blocks, 4):
                    strip = jnp.zeros((chan, tile), F32)
                    for block in range(first, min(first + 4, 9 * span)):
                        dz, dx = block // (3 * span), block // span % 3
                        dy = low + block % span - (part * half + y) + 1
                        if not 0 <= dy < 3:
                            continue
                        if back:
                            dz, dy, dx = 2 - dz, 2 - dy, 2 - dx
                        source = jnp.where(flip, 2 - dz, dz) if mirrored else dz
                        at = (dy * 3 + dx) * chan
                        tap = wide_ref[which, source, at : at + chan, :]
                        strip = jnp.where(group == block - first, tap, strip)
                    out[part, y * chan : (y + 1) * chan, first * chan : first * chan + tile] = (
                        strip.astype(BF16)
                    )


class Field:
    def __init__(self, pieces, full, width):
        self.pieces, self.full, self.width = pieces, full, width

    def run(self, plane, count):
        for ref, first, number, base in self.pieces:
            if first <= plane < first + number:
                at = plane - first
                size = min(count, number - at)
                return ref, slice((base + at) * self.width, (base + at + size) * self.width), size
        raise IndexError(plane)

    def take(self, rows, first, count):
        parts = []
        while count:
            ref, lanes, size = self.run(first, count)
            parts.append(ref[rows, lanes])
            first, count = first + size, count - size
        return parts[0] if len(parts) == 1 else jnp.concatenate(parts, axis=1)

    def put(self, plane, value):
        full, width = self.full, self.width
        ref, lanes, _ = self.run(plane, 1)
        lane = lax.broadcasted_iota(jnp.int32, (full, width), 1)
        before = jnp.where(lane == 0, 0.0, pltpu.roll(value, 1, 1))
        after = jnp.where(lane == width - 1, 0.0, pltpu.roll(value, width - 1, 1))
        for dx, item in enumerate((before, value, after)):
            ref[dx * full : (dx + 1) * full, lanes] = item.astype(BF16)

    def blank(self, plane):
        ref, lanes, _ = self.run(plane, 1)
        ref[:, lanes] = jnp.zeros((3 * self.full, self.width), BF16)

    def convolve(self, band, first, count, chan):
        half, span, lows, blocks = layout(self.full // chan)
        out = []
        for part, low in enumerate(lows):
            windows = [
                self.take(
                    slice(dx * self.full + low * chan, dx * self.full + (low + span) * chan),
                    first + dz - 1,
                    count,
                )
                for dz in range(3)
                for dx in range(3)
            ]
            if blocks > 9 * span:
                windows.append(self.take(slice(0, (blocks - 9 * span) * chan), first, count))
            window = jnp.concatenate(windows, axis=0)
            out.append(jnp.dot(band[part], window, preferred_element_type=F32))
        return jnp.concatenate(out, axis=0)


def spans(low, high):
    return [(at, min(2, high - at)) for at in range(low, high, 2)]


def sigmoid(value):
    return 0.5 * jnp.tanh(0.5 * value) + 0.5


def gradient(field, grads, own, chan, flip, out_ref):
    full = field.full
    height = full // chan
    sums = [[None] * 3 for _ in range(3)]
    for base in range(0, height, 2):
        right = jnp.concatenate(
            [
                grads.take(slice((2 - dx) * full + y * chan, (2 - dx) * full + (y + 1) * chan), 0, own)
                for y in (base, base + 1)
                for dx in (0, 1, 2, 2)
            ],
            axis=0,
        )
        low, high = max(base - 1, 0), min(base + 3, height)
        left = jnp.concatenate(
            [
                field.take(slice(full + low * chan, full + high * chan), dz - 1, own)
                for dz in range(3)
            ],
            axis=0,
        )
        piece = lax.dot_general(left, right, NT, preferred_element_type=F32)
        for dz in range(3):
            for step in range(2):
                for dy in range(3):
                    at = base + step + dy - 1
                    if 0 <= at < height:
                        row = (dz * (high - low) + at - low) * chan
                        part = piece[row : row + chan, step * 4 * chan : (step + 1) * 4 * chan]
                        held = sums[dz][dy]
                        sums[dz][dy] = part if held is None else held + part
    if flip is not None:
        first = [jnp.where(flip, c, a) for a, c in zip(sums[0], sums[2])]
        third = [jnp.where(flip, a, c) for a, c in zip(sums[0], sums[2])]
        sums = [first, sums[1], third]
    for dz in range(2):
        for dy in range(3):
            row = (dz * 3 + dy) * chan
            out_ref[row : row + chan, : 3 * chan] = sums[dz][dy][:, : 3 * chan]
            out_ref[row : row + chan, 3 * chan :] = sums[2][dy][:, dz * chan : (dz + 1) * chan]
    for dy in range(3):
        out_ref[6 * chan :, dy * chan : (dy + 1) * chan] = sums[2][dy][:, 2 * chan : 3 * chan]
    out_ref[6 * chan :, 3 * chan :] = jnp.zeros((chan, chan), F32)


def main_kernel(count, sizes, *refs):
    chan, own, height, width, low_side, high_side = sizes
    full = chan * height
    mirrored = count == 2
    halos = low_side + high_side
    data_ref, cot_ref = refs[:2]
    halo_refs = refs[2 : 2 + halos]
    band_one, band_two, back_two = refs[2 + halos : 5 + halos]
    grad_field_ref, term_one, term_two = refs[5 + halos : 8 + halos]
    edge_ref, h_ref, g_ref, slope_ref, turn_ref = refs[8 + halos :]
    position = lax.axis_index("gz")
    flip = position == 1 if mirrored else None

    def reach(depth):
        return (-depth * low_side, own + depth * high_side)

    def field(ref, depth):
        before = depth if low_side else 1
        item = Field([(ref, -before, slots(sizes, depth), 0)], full, width)
        return blanked(item)

    def blanked(item):
        if not low_side:
            item.blank(-1)
        if not high_side:
            item.blank(own)
        return item

    def plane_of(ref, plane, skip, depth):
        if 0 <= plane < own:
            at = jnp.where(flip, own - 1 - plane, plane) if mirrored else plane
            return ref[:, at]
        if plane < 0:
            return halo_refs[0][:, skip + depth + plane]
        at = plane - own
        if mirrored:
            at = jnp.where(flip, depth - 1 - at, at)
        return halo_refs[-1][:, skip + at]

    def kept(plane, value):
        if count == 2:
            return value
        if plane < 0:
            return jnp.where(position > 0, value, 0.0)
        if plane >= own:
            return jnp.where(position < count - 1, value, 0.0)
        return value

    before = REACH if low_side else 1
    after = REACH if high_side else 1
    data = Field(
        [(data_ref, 0, own, 0), (edge_ref, -before, before, 0), (edge_ref, own, after, before)],
        full,
        width,
    )
    blanked(data)
    for plane in range(*reach(REACH)):
        if not 0 <= plane < own:
            data.put(plane, turned(turn_ref, plane % 2, plane_of(None, plane, 0, REACH)))

    hidden = field(h_ref, REACH - 1)
    slope_low, slope_high = reach(1)
    for first, number in spans(*reach(REACH - 1)):
        pre = data.convolve(band_one, first, number, chan)
        for step in range(number):
            plane = first + step
            value = pre[:, step * width : (step + 1) * width]
            gate = sigmoid(value)
            hidden.put(plane, kept(plane, value * gate))
            if slope_low <= plane < slope_high:
                at = (plane - slope_low) * width
                slope_ref[:, at : at + width] = gate * (1.0 + value * (1.0 - gate))

    upper = field(g_ref, REACH - 2)
    for first, number in spans(*reach(REACH - 2)):
        pre = hidden.convolve(band_two, first, number, chan)
        for step in range(number):
            plane = first + step
            value = pre[:, step * width : (step + 1) * width]
            gate = sigmoid(value)
            seed = turned(turn_ref, plane % 2, plane_of(cot_ref, plane, REACH, REACH - 2))
            upper.put(plane, seed * (gate * (1.0 + value * (1.0 - gate))))

    lower = field(grad_field_ref, REACH - 3)
    for first, number in spans(*reach(REACH - 3)):
        back = upper.convolve(back_two, first, number, chan)
        for step in range(number):
            plane = first + step
            at = (plane - slope_low) * width
            grad = back[:, step * width : (step + 1) * width] * slope_ref[:, at : at + width]
            lower.put(plane, kept(plane, grad))
    gradient(hidden, upper, own, chan, flip, term_two)
    gradient(data, lower, own, chan, flip, term_one)


def slots(sizes, depth):
    _, own, _, _, low_side, high_side = sizes
    return own + sum(depth if side else 1 for side in (low_side, high_side))


def last_kernel(count, sizes, grad_field_ref, back_one, out_ref, turn_ref):
    chan, own, height, width, _, _ = sizes
    full = chan * height
    mirrored = count == 2
    flip = lax.axis_index("gz") == 1 if mirrored else None
    lower = Field([(grad_field_ref, -1, own + 2, 0)], full, width)
    for first, number in spans(0, own):
        out = lower.convolve(back_one, first, number, chan)
        for step in range(number):
            plane = first + step
            value = out[:, step * width : (step + 1) * width]
            slot = plane % 2
            for y in range(height):
                turn_ref[slot, pl.ds(y, chan, stride=height), :] = value[y * chan : (y + 1) * chan]
            at = jnp.where(flip, own - 1 - plane, plane) if mirrored else plane
            out_ref[:, at] = turn_ref[slot].reshape(chan, height, width).astype(BF16)


def holds_second():
    count, place, core = lax.axis_size("dp"), lax.axis_index("dp"), lax.axis_index("gz")
    for bit in range(count.bit_length() - 1):
        core = core + lax.shift_right_logical(place, bit)
    return core % 2 == 0


def unpack_kernel(factor, which, packed_ref, *refs):
    out_one, out_two, grad_ref, sem = refs[-4:]
    chan = grad_ref.shape[-1]
    value = packed_ref[...].T * factor
    for dz in range(3):
        for dy in range(3):
            for dx in range(3):
                row, column = (dx, 3 * dz + dy) if dz < 2 else (3, 3 * dx + dy)
                if dz == 2 and dx == 2:
                    row, column = dy, 6
                grad_ref[dz, dy, dx] = value[
                    row * chan : (row + 1) * chan, column * chan : (column + 1) * chan
                ]

    def send(out):
        copy = pltpu.make_async_copy(grad_ref, out, sem)
        copy.start()
        copy.wait()

    if which in (0, 1):
        send(out_two if which else out_one)
    else:
        second = holds_second() == (which == "held")
        pl.when(second)(lambda: send(out_two))
        pl.when(jnp.logical_not(second))(lambda: send(out_one))


def unpacked(packed, which, factor, chan, outs=()):
    shape = (3, 3, 3, chan, chan)
    hbm = pl.BlockSpec(memory_space=pltpu.HBM)
    return pl.pallas_call(
        functools.partial(unpack_kernel, factor, which),
        out_shape=[pltpu.HBM(shape, F32)] * 2,
        in_specs=[pl.BlockSpec(memory_space=pltpu.VMEM)] + [hbm] * len(outs),
        out_specs=[hbm] * 2,
        scratch_shapes=[pltpu.VMEM(shape, F32), pltpu.SemaphoreType.DMA],
        input_output_aliases={1 + k: k for k in range(len(outs))},
        compiler_params=params(8),
        cost_estimate=cost(1e9, 1e6),
        name="unpack",
    )(packed, *outs)


def doubled(value, axis):
    count = lax.axis_size(axis)
    if count & (count - 1):
        return lax.psum(value, axis)
    step = 1
    while step < count:
        value = value + lax.ppermute(value, axis, [(i, i ^ step) for i in range(count)])
        step *= 2
    return value


def odd(index):
    return bin(index).count("1") % 2


def crossed(value, before_last):
    count = lax.axis_size("dp")
    steps = [1 << k for k in range(count.bit_length() - 1)]
    near, far = steps[:-1], steps[-1:]
    orders = (near[:1] + far + near[1:], near[-1:] + near[:1] + far + near[1:-1])
    if len(steps) < 3:
        orders = (steps, steps)
    for phase in range(len(steps)):
        if phase == len(steps) - 1:
            value = before_last(value)
        sent = value.astype(BF16)
        moves = []
        for core in range(2):
            for chip in range(count):
                step = orders[core ^ odd(chip)][phase]
                moves.append((core * count + chip, (1 - core) * count + (chip ^ step)))
        value = sent.astype(F32) + lax.ppermute(sent, ("gz", "dp"), moves).astype(F32)
    return value


def reduced(one, two, grad_fields, finish, unpack):
    outs = []

    def gate(value):
        value, *held = lax.optimization_barrier((value, *grad_fields))
        outs.extend(finish(held))
        return value

    count = lax.axis_size("dp")
    if lax.axis_size("gz") == 2 and count > 1 and count & (count - 1) == 0:
        swap = [(0, 1), (1, 0)]
        second = holds_second()
        mine = jnp.where(second, two, one)
        mine = mine + lax.ppermute(jnp.where(second, one, two), "gz", swap)
        mine = crossed(mine, gate)
        mine, *outs = lax.optimization_barrier((mine, *outs))
        other = lax.ppermute(mine, "gz", swap)
        return unpack(other, "other", unpack(mine, "held")), outs
    both = doubled(doubled(jnp.stack([one, two]), "gz"), "dp")
    return unpack(both[1], 1, unpack(both[0], 0)), finish(grad_fields)


def gathered(count, data, cot, *taps):
    chan, own, height, width = data.shape
    sides = min(count - 1, 2)
    arrays = (data, cot, *taps)
    far = [pltpu.with_memory_space_constraint(value, pltpu.HBM) for value in arrays]
    shapes = [value.shape for value in (data, *taps)]
    shapes += [(chan, 2 * REACH - 2, height, width)] * sides
    near = pl.pallas_call(
        functools.partial(pack_kernel, count, own),
        out_shape=[pltpu.VMEM(shape, BF16) for shape in shapes],
        in_specs=[pl.BlockSpec(memory_space=pltpu.HBM)] * 4,
        out_specs=[pl.BlockSpec(memory_space=pltpu.VMEM)] * len(shapes),
        scratch_shapes=[pltpu.SemaphoreType.DMA((3 + 2 * sides,))],
        compiler_params=params(4),
        name="pack",
    )(*far)
    messages = near[3:]
    if count == 2:
        moves = [[(0, 1), (1, 0)]]
    else:
        up = [(i, i + 1) for i in range(count - 1)]
        moves = [up, [(j, i) for i, j in up]]
    return [near[0], cot, *near[1:3]], [lax.ppermute(item, "gz", move) for item, move in zip(messages, moves)]


def local(inputs, kernel_one, kernel_two, cotangent):
    count = lax.axis_size("gz")
    batch, chan, own, height, width = inputs.shape
    full = chan * height
    low_side, high_side = (1, 1) if count > 2 else (0, 1 if count == 2 else 0)
    sizes = (chan, own, height, width, low_side, high_side)
    taps = [jnp.transpose(k, (2, 3, 4, 0, 1)) for k in (kernel_one, kernel_two)]
    turn = pltpu.VMEM((2, full, width), F32)
    half, _, _, blocks = layout(height)

    def stack(depth):
        return (3 * full, slots(sizes, depth) * width)

    grad_fields, backs, ones, twos = [], [], [], []
    for sample in range(batch):
        near, halos = gathered(count, inputs[sample], cotangent[sample], *taps)
        data, cot, *near_taps = near
        *bands, field = pl.pallas_call(
            functools.partial(prep_kernel, count == 2),
            out_shape=[jax.ShapeDtypeStruct((2, half * chan, blocks * chan), BF16)] * 4
            + [jax.ShapeDtypeStruct((3 * full, own * width), BF16)],
            scratch_shapes=[pltpu.VMEM((4, 3, 9 * chan, 4 * chan), F32), turn],
            compiler_params=params(16),
            cost_estimate=cost(2e9, 5e6),
            name="prep",
        )(data, *near_taps)
        term = jax.ShapeDtypeStruct((7 * chan, 4 * chan), F32)
        grad_field, term_one, term_two = pl.pallas_call(
            functools.partial(main_kernel, count, sizes),
            out_shape=[jax.ShapeDtypeStruct(stack(REACH - 3), BF16), term, term],
            scratch_shapes=[
                pltpu.VMEM((3 * full, (slots(sizes, REACH) - own) * width), BF16),
                pltpu.VMEM(stack(REACH - 1), BF16),
                pltpu.VMEM(stack(REACH - 2), BF16),
                pltpu.VMEM((full, (own + low_side + high_side) * width), F32),
                turn,
            ],
            compiler_params=params(32),
            cost_estimate=cost(8e9, 8e6),
            name="main",
        )(field, cot, *halos, bands[0], bands[2], bands[3])
        grad_fields.append(grad_field)
        backs.append(bands[1])
        ones.append(term_one)
        twos.append(term_two)

    def finish(fields):
        return [
            pl.pallas_call(
                functools.partial(last_kernel, count, sizes),
                out_shape=jax.ShapeDtypeStruct((chan, own, height, width), BF16),
                scratch_shapes=[turn],
                compiler_params=params(16),
                cost_estimate=cost(2e9, 3e6),
                name="last",
            )(*pair)
            for pair in zip(fields, backs)
        ]

    cells = lax.axis_size("dp") * batch * count * own * height * width

    def unpack(packed, which, outs=()):
        return unpacked(packed, which, 1.0 / math.sqrt(cells), chan, outs)

    one, two = sum(ones[1:], ones[0]), sum(twos[1:], twos[0])
    grads, outs = reduced(one, two, grad_fields, finish, unpack)
    one, two = [jnp.transpose(g, (3, 4, 0, 1, 2)) for g in grads]
    return jnp.stack(outs), one, two


def solution(mesh):
    return jax.shard_map(
        local,
        mesh=mesh,
        in_specs=(P("dp", None, "gz", None, None), P(), P(), P("dp", None, "gz", None, None)),
        out_specs=(P("dp", None, "gz", None, None), P(), P()),
        check_vma=False,
    )
```

```python
import functools
import math

import jax
import jax.numpy as jnp
from jax import lax
from jax.experimental import pallas as pl
from jax.experimental.pallas import tpu as pltpu
from jax.sharding import PartitionSpec as P

F32, BF16 = jnp.float32, jnp.bfloat16
NT = (((1,), (1,)), ((), ()))
REACH = 4


def params(mib):
    return pltpu.CompilerParams(vmem_limit_bytes=mib * 2**20)


def cost(flops, size):
    return pl.CostEstimate(flops=int(flops), bytes_accessed=int(size), transcendentals=0)


def pack_kernel(count, own, *refs):
    sources, near, outs, sems = refs[:4], refs[4:7], refs[7:-1], refs[-1]
    pairs = []
    for side, out in enumerate(outs):
        for ref, depth, at in ((sources[0], REACH, 0), (sources[1], REACH - 2, REACH)):
            start = own - depth if side == 0 else 0
            if count == 2:
                start = jnp.where(lax.axis_index("gz") == 1, 0, own - depth)
            pairs.append((ref.at[:, pl.ds(start, depth)], out.at[:, pl.ds(at, depth)]))
    pairs.extend(zip((sources[0], *sources[2:]), near))
    copies = [pltpu.make_async_copy(*pair, sems.at[k]) for k, pair in enumerate(pairs)]
    for copy in copies:
        copy.start()
    for copy in copies:
        copy.wait()


def turned(turn_ref, slot, value):
    chan, height, width = value.shape
    turn_ref[slot] = value.astype(F32).reshape(chan * height, width)
    return jnp.concatenate(
        [turn_ref[slot, pl.ds(y, chan, stride=height), :] for y in range(height)], axis=0
    )


def layout(height):
    half = height // 2
    span = half + 1
    return half, span, (0, half - 1), -(-9 * span // 8) * 8


def prep_kernel(mirrored, data_ref, one_ref, two_ref, *refs):
    flip = lax.axis_index("gz") == 1 if mirrored else False
    outs, field_ref, wide_ref, turn_ref = refs[:4], refs[4], refs[5], refs[6]
    chan = one_ref.shape[-1]
    own, height, width = data_ref.shape[1:]
    full = chan * height
    field = Field([(field_ref, 0, own, 0)], full, width)
    for plane in range(own):
        at = jnp.where(flip, own - 1 - plane, plane) if mirrored else plane
        field.put(plane, turned(turn_ref, plane % 2, data_ref[:, at]))

    def iota(shape, dim):
        return lax.broadcasted_iota(jnp.int32, shape, dim)

    tile = 4 * chan
    same = lax.rem(iota((chan, tile), 1), chan) == iota((chan, tile), 0)
    repeat = jnp.where(same, 1.0, 0.0).astype(BF16)
    unit = jnp.where(iota((chan, chan), 0) == iota((chan, chan), 1), 1.0, 0.0).astype(BF16)
    row, lane = iota((tile, 4 * tile), 0), iota((tile, 4 * tile), 1)
    chosen = (row // chan == lane // tile) & (lax.rem(row, chan) == lax.rem(lane, chan))
    choose = jnp.where(chosen, 1.0, 0.0).astype(BF16)
    group = iota((chan, tile), 1) // chan
    half, span, lows, blocks = layout(height)
    for index, ref in enumerate((one_ref, two_ref)):
        flat = ref[...].reshape(27 * chan, chan)
        spread = jnp.dot(flat, repeat, preferred_element_type=F32)
        wide_ref[2 * index] = spread.reshape(3, 9 * chan, tile)
        flat = jnp.concatenate([flat, jnp.zeros((chan, chan), BF16)], axis=0)
        across = lax.dot_general(unit, flat, NT, preferred_element_type=F32).astype(BF16)
        stacked = jnp.concatenate([across[:, t * tile : (t + 1) * tile] for t in range(7)], axis=0)
        spread = jnp.dot(stacked, choose, preferred_element_type=F32)
        for tap in range(27):
            at, column = tap // 4 * chan, tap % 4 * tile
            wide_ref[2 * index + 1, tap // 9, tap % 9 * chan : (tap % 9 + 1) * chan] = spread[
                at : at + chan, column : column + tile
            ]
    for which, out in enumerate(outs):
        back = which % 2
        for part, low in enumerate(lows):
            for y in range(half):
                for first in range(0, blocks, 4):
                    strip = jnp.zeros((chan, tile), F32)
                    for block in range(first, min(first + 4, 9 * span)):
                        dz, dx = block // (3 * span), block // span % 3
                        dy = low + block % span - (part * half + y) + 1
                        if not 0 <= dy < 3:
                            continue
                        if back:
                            dz, dy, dx = 2 - dz, 2 - dy, 2 - dx
                        source = jnp.where(flip, 2 - dz, dz) if mirrored else dz
                        at = (dy * 3 + dx) * chan
                        tap = wide_ref[which, source, at : at + chan, :]
                        strip = jnp.where(group == block - first, tap, strip)
                    out[part, y * chan : (y + 1) * chan, first * chan : first * chan + tile] = (
                        strip.astype(BF16)
                    )


class Field:
    def __init__(self, pieces, full, width):
        self.pieces, self.full, self.width = pieces, full, width

    def run(self, plane, count):
        for ref, first, number, base in self.pieces:
            if first <= plane < first + number:
                at = plane - first
                size = min(count, number - at)
                return ref, slice((base + at) * self.width, (base + at + size) * self.width), size
        raise IndexError(plane)

    def take(self, rows, first, count):
        parts = []
        while count:
            ref, lanes, size = self.run(first, count)
            parts.append(ref[rows, lanes])
            first, count = first + size, count - size
        return parts[0] if len(parts) == 1 else jnp.concatenate(parts, axis=1)

    def put(self, plane, value):
        full, width = self.full, self.width
        ref, lanes, _ = self.run(plane, 1)
        lane = lax.broadcasted_iota(jnp.int32, (full, width), 1)
        before = jnp.where(lane == 0, 0.0, pltpu.roll(value, 1, 1))
        after = jnp.where(lane == width - 1, 0.0, pltpu.roll(value, width - 1, 1))
        for dx, item in enumerate((before, value, after)):
            ref[dx * full : (dx + 1) * full, lanes] = item.astype(BF16)

    def blank(self, plane):
        ref, lanes, _ = self.run(plane, 1)
        ref[:, lanes] = jnp.zeros((3 * self.full, self.width), BF16)

    def convolve(self, band, first, count, chan):
        half, span, lows, blocks = layout(self.full // chan)
        out = []
        for part, low in enumerate(lows):
            windows = [
                self.take(
                    slice(dx * self.full + low * chan, dx * self.full + (low + span) * chan),
                    first + dz - 1,
                    count,
                )
                for dz in range(3)
                for dx in range(3)
            ]
            if blocks > 9 * span:
                windows.append(self.take(slice(0, (blocks - 9 * span) * chan), first, count))
            window = jnp.concatenate(windows, axis=0)
            out.append(jnp.dot(band[part], window, preferred_element_type=F32))
        return jnp.concatenate(out, axis=0)


def spans(low, high):
    return [(at, min(2, high - at)) for at in range(low, high, 2)]


def sigmoid(value):
    return 0.5 * jnp.tanh(0.5 * value) + 0.5


def gradient(field, grads, own, chan, flip, out_ref):
    full = field.full
    height = full // chan
    sums = [[None] * 3 for _ in range(3)]
    for base in range(0, height, 2):
        right = jnp.concatenate(
            [
                grads.take(slice((2 - dx) * full + y * chan, (2 - dx) * full + (y + 1) * chan), 0, own)
                for y in (base, base + 1)
                for dx in (0, 1, 2, 2)
            ],
            axis=0,
        )
        low, high = max(base - 1, 0), min(base + 3, height)
        left = jnp.concatenate(
            [
                field.take(slice(full + low * chan, full + high * chan), dz - 1, own)
                for dz in range(3)
            ],
            axis=0,
        )
        piece = lax.dot_general(left, right, NT, preferred_element_type=F32)
        for dz in range(3):
            for step in range(2):
                for dy in range(3):
                    at = base + step + dy - 1
                    if 0 <= at < height:
                        row = (dz * (high - low) + at - low) * chan
                        part = piece[row : row + chan, step * 4 * chan : (step + 1) * 4 * chan]
                        held = sums[dz][dy]
                        sums[dz][dy] = part if held is None else held + part
    if flip is not None:
        first = [jnp.where(flip, c, a) for a, c in zip(sums[0], sums[2])]
        third = [jnp.where(flip, a, c) for a, c in zip(sums[0], sums[2])]
        sums = [first, sums[1], third]
    for dz in range(2):
        for dy in range(3):
            row = (dz * 3 + dy) * chan
            out_ref[row : row + chan, : 3 * chan] = sums[dz][dy][:, : 3 * chan]
            out_ref[row : row + chan, 3 * chan :] = sums[2][dy][:, dz * chan : (dz + 1) * chan]
    for dy in range(3):
        out_ref[6 * chan :, dy * chan : (dy + 1) * chan] = sums[2][dy][:, 2 * chan : 3 * chan]
    out_ref[6 * chan :, 3 * chan :] = jnp.zeros((chan, chan), F32)


def main_kernel(count, sizes, *refs):
    chan, own, height, width, low_side, high_side = sizes
    full = chan * height
    mirrored = count == 2
    halos = low_side + high_side
    data_ref, cot_ref = refs[:2]
    halo_refs = refs[2 : 2 + halos]
    band_one, band_two, back_two = refs[2 + halos : 5 + halos]
    grad_field_ref, term_one, term_two = refs[5 + halos : 8 + halos]
    edge_ref, h_ref, g_ref, slope_ref, turn_ref = refs[8 + halos :]
    position = lax.axis_index("gz")
    flip = position == 1 if mirrored else None

    def reach(depth):
        return (-depth * low_side, own + depth * high_side)

    def field(ref, depth):
        before = depth if low_side else 1
        item = Field([(ref, -before, slots(sizes, depth), 0)], full, width)
        return blanked(item)

    def blanked(item):
        if not low_side:
            item.blank(-1)
        if not high_side:
            item.blank(own)
        return item

    def plane_of(ref, plane, skip, depth):
        if 0 <= plane < own:
            at = jnp.where(flip, own - 1 - plane, plane) if mirrored else plane
            return ref[:, at]
        if plane < 0:
            return halo_refs[0][:, skip + depth + plane]
        at = plane - own
        if mirrored:
            at = jnp.where(flip, depth - 1 - at, at)
        return halo_refs[-1][:, skip + at]

    def kept(plane, value):
        if count == 2:
            return value
        if plane < 0:
            return jnp.where(position > 0, value, 0.0)
        if plane >= own:
            return jnp.where(position < count - 1, value, 0.0)
        return value

    before = REACH if low_side else 1
    after = REACH if high_side else 1
    data = Field(
        [(data_ref, 0, own, 0), (edge_ref, -before, before, 0), (edge_ref, own, after, before)],
        full,
        width,
    )
    blanked(data)
    for plane in range(*reach(REACH)):
        if not 0 <= plane < own:
            data.put(plane, turned(turn_ref, plane % 2, plane_of(None, plane, 0, REACH)))

    hidden = field(h_ref, REACH - 1)
    slope_low, slope_high = reach(1)
    for first, number in spans(*reach(REACH - 1)):
        pre = data.convolve(band_one, first, number, chan)
        for step in range(number):
            plane = first + step
            value = pre[:, step * width : (step + 1) * width]
            gate = sigmoid(value)
            hidden.put(plane, kept(plane, value * gate))
            if slope_low <= plane < slope_high:
                at = (plane - slope_low) * width
                slope_ref[:, at : at + width] = gate * (1.0 + value * (1.0 - gate))

    upper = field(g_ref, REACH - 2)
    for first, number in spans(*reach(REACH - 2)):
        pre = hidden.convolve(band_two, first, number, chan)
        for step in range(number):
            plane = first + step
            value = pre[:, step * width : (step + 1) * width]
            gate = sigmoid(value)
            seed = turned(turn_ref, plane % 2, plane_of(cot_ref, plane, REACH, REACH - 2))
            upper.put(plane, seed * (gate * (1.0 + value * (1.0 - gate))))

    lower = field(grad_field_ref, REACH - 3)
    for first, number in spans(*reach(REACH - 3)):
        back = upper.convolve(back_two, first, number, chan)
        for step in range(number):
            plane = first + step
            at = (plane - slope_low) * width
            grad = back[:, step * width : (step + 1) * width] * slope_ref[:, at : at + width]
            lower.put(plane, kept(plane, grad))
    gradient(hidden, upper, own, chan, flip, term_two)
    gradient(data, lower, own, chan, flip, term_one)


def slots(sizes, depth):
    _, own, _, _, low_side, high_side = sizes
    return own + sum(depth if side else 1 for side in (low_side, high_side))


def last_kernel(count, sizes, grad_field_ref, back_one, out_ref, turn_ref):
    chan, own, height, width, _, _ = sizes
    full = chan * height
    mirrored = count == 2
    flip = lax.axis_index("gz") == 1 if mirrored else None
    lower = Field([(grad_field_ref, -1, own + 2, 0)], full, width)
    for first, number in spans(0, own):
        out = lower.convolve(back_one, first, number, chan)
        for step in range(number):
            plane = first + step
            value = out[:, step * width : (step + 1) * width]
            slot = plane % 2
            for y in range(height):
                turn_ref[slot, pl.ds(y, chan, stride=height), :] = value[y * chan : (y + 1) * chan]
            at = jnp.where(flip, own - 1 - plane, plane) if mirrored else plane
            out_ref[:, at] = turn_ref[slot].reshape(chan, height, width).astype(BF16)


def holds_second():
    count, place, core = lax.axis_size("dp"), lax.axis_index("dp"), lax.axis_index("gz")
    for bit in range(count.bit_length() - 1):
        core = core + lax.shift_right_logical(place, bit)
    return core % 2 == 0


def unpack_kernel(factor, which, packed_ref, *refs):
    out_one, out_two, grad_ref, sem = refs[-4:]
    chan = grad_ref.shape[-1]
    value = packed_ref[...].T * factor

    def each(dz, act):
        def on(out):
            act(pltpu.make_async_copy(grad_ref.at[dz], out.at[dz], sem.at[dz]))

        if which in (0, 1):
            on(out_two if which else out_one)
        else:
            second = holds_second() == (which == "held")
            pl.when(second)(lambda: on(out_two))
            pl.when(jnp.logical_not(second))(lambda: on(out_one))

    for dz in range(3):
        for dy in range(3):
            for dx in range(3):
                row, column = (dx, 3 * dz + dy) if dz < 2 else (3, 3 * dx + dy)
                if dz == 2 and dx == 2:
                    row, column = dy, 6
                grad_ref[dz, dy, dx] = value[
                    row * chan : (row + 1) * chan, column * chan : (column + 1) * chan
                ]
        each(dz, lambda copy: copy.start())
    for dz in range(3):
        each(dz, lambda copy: copy.wait())


def unpacked(packed, which, factor, chan, outs=()):
    shape = (3, 3, 3, chan, chan)
    hbm = pl.BlockSpec(memory_space=pltpu.HBM)
    return pl.pallas_call(
        functools.partial(unpack_kernel, factor, which),
        out_shape=[pltpu.HBM(shape, F32)] * 2,
        in_specs=[pl.BlockSpec(memory_space=pltpu.VMEM)] + [hbm] * len(outs),
        out_specs=[hbm] * 2,
        scratch_shapes=[pltpu.VMEM(shape, F32), pltpu.SemaphoreType.DMA((3,))],
        input_output_aliases={1 + k: k for k in range(len(outs))},
        compiler_params=params(8),
        cost_estimate=cost(1e9, 1e6),
        name="unpack",
    )(packed, *outs)


def doubled(value, axis):
    count = lax.axis_size(axis)
    if count & (count - 1):
        return lax.psum(value, axis)
    step = 1
    while step < count:
        value = value + lax.ppermute(value, axis, [(i, i ^ step) for i in range(count)])
        step *= 2
    return value


def odd(index):
    return bin(index).count("1") % 2


def crossed(value, before_last):
    count = lax.axis_size("dp")
    steps = [1 << k for k in range(count.bit_length() - 1)]
    near, far = steps[:-1], steps[-1:]
    orders = (near[:1] + far + near[1:], near[-1:] + near[:1] + far + near[1:-1])
    if len(steps) < 3:
        orders = (steps, steps)
    for phase in range(len(steps)):
        if phase == len(steps) - 1:
            value = before_last(value)
        sent = value.astype(BF16)
        moves = []
        for core in range(2):
            for chip in range(count):
                step = orders[core ^ odd(chip)][phase]
                moves.append((core * count + chip, (1 - core) * count + (chip ^ step)))
        value = sent.astype(F32) + lax.ppermute(sent, ("gz", "dp"), moves).astype(F32)
    return value


def reduced(one, two, grad_fields, finish, unpack):
    outs = []

    def gate(value):
        value, *held = lax.optimization_barrier((value, *grad_fields))
        outs.extend(finish(held))
        return value

    count = lax.axis_size("dp")
    if lax.axis_size("gz") == 2 and count > 1 and count & (count - 1) == 0:
        swap = [(0, 1), (1, 0)]
        second = holds_second()
        mine = jnp.where(second, two, one)
        mine = mine + lax.ppermute(jnp.where(second, one, two), "gz", swap)
        mine = crossed(mine, gate)
        mine, *outs = lax.optimization_barrier((mine, *outs))
        other = lax.ppermute(mine, "gz", swap)
        return unpack(other, "other", unpack(mine, "held")), outs
    both = doubled(doubled(jnp.stack([one, two]), "gz"), "dp")
    return unpack(both[1], 1, unpack(both[0], 0)), finish(grad_fields)


def gathered(count, data, cot, *taps):
    chan, own, height, width = data.shape
    sides = min(count - 1, 2)
    arrays = (data, cot, *taps)
    far = [pltpu.with_memory_space_constraint(value, pltpu.HBM) for value in arrays]
    shapes = [value.shape for value in (data, *taps)]
    shapes += [(chan, 2 * REACH - 2, height, width)] * sides
    near = pl.pallas_call(
        functools.partial(pack_kernel, count, own),
        out_shape=[pltpu.VMEM(shape, BF16) for shape in shapes],
        in_specs=[pl.BlockSpec(memory_space=pltpu.HBM)] * 4,
        out_specs=[pl.BlockSpec(memory_space=pltpu.VMEM)] * len(shapes),
        scratch_shapes=[pltpu.SemaphoreType.DMA((3 + 2 * sides,))],
        compiler_params=params(4),
        name="pack",
    )(*far)
    messages = near[3:]
    if count == 2:
        moves = [[(0, 1), (1, 0)]]
    else:
        up = [(i, i + 1) for i in range(count - 1)]
        moves = [up, [(j, i) for i, j in up]]
    return [near[0], cot, *near[1:3]], [lax.ppermute(item, "gz", move) for item, move in zip(messages, moves)]


def local(inputs, kernel_one, kernel_two, cotangent):
    count = lax.axis_size("gz")
    batch, chan, own, height, width = inputs.shape
    full = chan * height
    low_side, high_side = (1, 1) if count > 2 else (0, 1 if count == 2 else 0)
    sizes = (chan, own, height, width, low_side, high_side)
    taps = [jnp.transpose(k, (2, 3, 4, 0, 1)) for k in (kernel_one, kernel_two)]
    turn = pltpu.VMEM((2, full, width), F32)
    half, _, _, blocks = layout(height)

    def stack(depth):
        return (3 * full, slots(sizes, depth) * width)

    grad_fields, backs, ones, twos = [], [], [], []
    for sample in range(batch):
        near, halos = gathered(count, inputs[sample], cotangent[sample], *taps)
        data, cot, *near_taps = near
        *bands, field = pl.pallas_call(
            functools.partial(prep_kernel, count == 2),
            out_shape=[jax.ShapeDtypeStruct((2, half * chan, blocks * chan), BF16)] * 4
            + [jax.ShapeDtypeStruct((3 * full, own * width), BF16)],
            scratch_shapes=[pltpu.VMEM((4, 3, 9 * chan, 4 * chan), F32), turn],
            compiler_params=params(16),
            cost_estimate=cost(2e9, 5e6),
            name="prep",
        )(data, *near_taps)
        term = jax.ShapeDtypeStruct((7 * chan, 4 * chan), F32)
        grad_field, term_one, term_two = pl.pallas_call(
            functools.partial(main_kernel, count, sizes),
            out_shape=[jax.ShapeDtypeStruct(stack(REACH - 3), BF16), term, term],
            scratch_shapes=[
                pltpu.VMEM((3 * full, (slots(sizes, REACH) - own) * width), BF16),
                pltpu.VMEM(stack(REACH - 1), BF16),
                pltpu.VMEM(stack(REACH - 2), BF16),
                pltpu.VMEM((full, (own + low_side + high_side) * width), F32),
                turn,
            ],
            compiler_params=params(32),
            cost_estimate=cost(8e9, 8e6),
            name="main",
        )(field, cot, *halos, bands[0], bands[2], bands[3])
        grad_fields.append(grad_field)
        backs.append(bands[1])
        ones.append(term_one)
        twos.append(term_two)

    def finish(fields):
        return [
            pl.pallas_call(
                functools.partial(last_kernel, count, sizes),
                out_shape=jax.ShapeDtypeStruct((chan, own, height, width), BF16),
                scratch_shapes=[turn],
                compiler_params=params(16),
                cost_estimate=cost(2e9, 3e6),
                name="last",
            )(*pair)
            for pair in zip(fields, backs)
        ]

    cells = lax.axis_size("dp") * batch * count * own * height * width

    def unpack(packed, which, outs=()):
        return unpacked(packed, which, 1.0 / math.sqrt(cells), chan, outs)

    one, two = sum(ones[1:], ones[0]), sum(twos[1:], twos[0])
    grads, outs = reduced(one, two, grad_fields, finish, unpack)
    one, two = [jnp.transpose(g, (3, 4, 0, 1, 2)) for g in grads]
    return jnp.stack(outs), one, two


def solution(mesh):
    return jax.shard_map(
        local,
        mesh=mesh,
        in_specs=(P("dp", None, "gz", None, None), P(), P(), P("dp", None, "gz", None, None)),
        out_specs=(P("dp", None, "gz", None, None), P(), P()),
        check_vma=False,
    )
```
